32 devices in a mesh: req: 16 (over z, y, x), tp: 2 (over core).
Axes of the slice: x: 2, y: 2, z: 4, core: 2. Of those that a mesh axis runs over, the one named last changes fastest.
Arguments:
- tokens: bfloat16 [8192, 1664], P('req'), may hold values from -6 to 6
- qkv_weight: bfloat16 [1664, 3, 1664], P('req', None, 'tp')
- out_weight: bfloat16 [1664, 1664], P('tp', 'req'), may hold values from -0.15625 to 0.15625
- fc1_weight: bfloat16 [1664, 8192], P('req', 'tp'), may hold values from -0.15625 to 0.15625
- fc2_weight: bfloat16 [8192, 1664], P('tp', 'req'), may hold values from -0.0625 to 0.0625
- norm1_gain: float32 [1664], replicated, may hold values from 0.1 to 1.9
- norm2_gain: float32 [1664], replicated, may hold values from 0.1 to 1.9
- norm3_gain: float32 [1664], replicated, may hold values from 0.1 to 1.9
- proj_weight: bfloat16 [6656, 4096], P('req', 'tp'), may hold values from -0.078125 to 0.078125
- grid_h: int32 [32], replicated, may hold values from 2 to 16, as said below
- grid_w: int32 [32], replicated, may hold values from 2 to 16, as said below
- segment_ids: int32 [8192], P('req'), may hold values from 0 to 2, as said below
- patch_mask: int32 [8192], P('req'), may hold values from 0 to 1, as said below
- owner: int32 [32], replicated, may hold values from 0 to 15, as said below
Outputs:
- embedded: bfloat16 [2048, 4096], P('req', 'tp')
- pooled_norm: float32 [32], P('req')
- top_logit: float32 [32], P('req')
The draws below stay inside these ranges and needn't reach their ends.
Inputs may be any that keep to these rules, and one draw needn't show every extreme that they name: `grid_h`: Even. On one req index every request has height 16 and width 16, so that its requests fill all 512 rows. `grid_w`: Even. `segment_ids`: within the 512 rows of each req index, the j-th request of that index covers the next grid_h * grid_w rows with id j, from the first row on; the remaining rows carry id 2. `patch_mask`: 0 on every row with segment id 2. `owner`: the 2 requests of req index i are owned by the indices (i + o) mod the req axis's size, each o from 0 to 1 once.
All inputs are finite; a program needn't handle non-finite values.
Results may differ from the reference program's by a relative error of at most 0.0085.
The reference program's roundings to bfloat16 on the way count: a program that leaves them out, or rounds other values in their place, can miss the bound.
Values may be sent and summed in bfloat16 or wider, within the bound.
A program may use at most 128 MiB of HBM per device.

```python
import math
import jax
import jax.numpy as jnp
from jax import lax

D = 1664
HD = 104
FF = 8192
OUT = 4096
GH_MAX = 16
GW_MAX = 16
REQ_DEV = 2
TOK_DEV = 512
MCAP = 64
MERGED = 6656
REQUESTS = 32
TOKENS = 8192


def layout(key):
    devices = REQUESTS // REQ_DEV
    keys = jax.random.split(jax.random.fold_in(key, 7), 5)
    heights = 2 * jax.random.randint(keys[0], (devices, REQ_DEV), 1, GH_MAX // 2 + 1)
    widths = 2 * jax.random.randint(keys[1], (devices, REQ_DEV), 1, GW_MAX // 2 + 1)
    chosen = jax.random.randint(keys[2], (), 0, devices)
    filled = (jnp.arange(devices) == chosen)[:, None]
    heights = jnp.where(filled, GH_MAX, heights).astype(jnp.int32)
    widths = jnp.where(filled, GW_MAX, widths).astype(jnp.int32)
    ends = jnp.cumsum(heights * widths, axis=1)
    places = jnp.arange(TOK_DEV)
    segs = jnp.sum((places[None, None, :] >= ends[:, :, None]).astype(jnp.int32), axis=1)
    keep = (jax.random.randint(keys[3], (devices, TOK_DEV), 0, 8) > 0) & (segs < REQ_DEV)
    ranks = jax.random.randint(keys[4], (devices, REQ_DEV), 0, 1024) * REQ_DEV + jnp.arange(REQ_DEV)[None, :]
    order = jnp.argsort(ranks, axis=1)
    owners = jnp.mod(jnp.arange(devices)[:, None] + order, devices)
    return (heights.reshape(-1), widths.reshape(-1), segs.reshape(-1).astype(jnp.int32), keep.astype(jnp.int32).reshape(-1), owners.reshape(-1).astype(jnp.int32))


def draw_grid_h(key, part):
    return layout(key)[0]


def draw_grid_w(key, part):
    return layout(key)[1]


def draw_segment_ids(key, part):
    return layout(key)[2]


def draw_patch_mask(key, part):
    return layout(key)[3]


def draw_owner(key, part):
    return layout(key)[4]


def draw_qkv_weight(key, part):
    values = jax.random.normal(key, (D, 3, D), jnp.float32) * D ** (-0.5)
    return values.astype(jnp.bfloat16)


def level_of(rng, extent, cuts, low, high):
    level = 1.0
    for dim, parts in cuts:
        steps = jax.random.uniform(jax.random.fold_in(jax.random.fold_in(rng, 6), dim), (parts,), jnp.float32, low / len(cuts), high / len(cuts))
        level = level * jnp.repeat(jnp.exp(steps), extent[dim] // parts).reshape((-1,) + (1,) * (len(extent) - 1 - dim))
    return level


def normal_values(rng, shape, scale, most, shards=(), kind=jnp.bfloat16):
    level = level_of(rng, shape, shards, -0.22, 0.18) if shards else 1.0
    result = jax.random.normal(rng, shape, jnp.float32) * scale * level
    return jnp.minimum(jnp.maximum(result, -most), most).astype(kind)


def setup_inputs(seed: int = 0) -> dict:
    seeds = jax.random.split(jax.random.key(seed), 15)
    tokens = normal_values(seeds[0], (TOKENS, D), 1.0, 6.0, ((0, 16),))
    qkv_weight = draw_qkv_weight(jax.random.fold_in(seeds[14], 71), 0)
    out_weight = normal_values(seeds[2], (D, D), D ** -0.5, 0.15625, ((0, 2), (1, 16)))
    fc1_weight = normal_values(seeds[3], (D, FF), D ** -0.5, 0.15625, ((0, 16), (1, 2)))
    fc2_weight = normal_values(seeds[4], (FF, D), FF ** -0.5, 0.0625, ((0, 2), (1, 16)))
    norm1_gain = jnp.clip(1.0 + 0.18 * jax.random.normal(seeds[5], (D,), jnp.float32), 0.1, 1.9)
    norm2_gain = jnp.clip(1.0 + 0.18 * jax.random.normal(seeds[6], (D,), jnp.float32), 0.1, 1.9)
    norm3_gain = jnp.clip(1.0 + 0.18 * jax.random.normal(seeds[7], (D,), jnp.float32), 0.1, 1.9)
    proj_weight = normal_values(seeds[8], (MERGED, OUT), MERGED ** -0.5, 0.078125, ((0, 16), (1, 2)))
    grid_h = draw_grid_h(jax.random.fold_in(seeds[14], 71), 0)
    grid_w = draw_grid_w(jax.random.fold_in(seeds[14], 71), 0)
    segment_ids = draw_segment_ids(jax.random.fold_in(seeds[14], 71), 0)
    patch_mask = draw_patch_mask(jax.random.fold_in(seeds[14], 71), 0)
    owner = draw_owner(jax.random.fold_in(seeds[14], 71), 0)
    return {"tokens": tokens, "qkv_weight": qkv_weight, "out_weight": out_weight, "fc1_weight": fc1_weight, "fc2_weight": fc2_weight, "norm1_gain": norm1_gain, "norm2_gain": norm2_gain, "norm3_gain": norm3_gain, "proj_weight": proj_weight, "grid_h": grid_h, "grid_w": grid_w, "segment_ids": segment_ids, "patch_mask": patch_mask, "owner": owner}


EPS = 1e-06

def layer_norm(rows, gain):
    mean = lax.optimization_barrier(jnp.mean(rows, axis=-1, keepdims=True))
    centered = rows - mean
    spread = lax.optimization_barrier(jnp.mean(centered * centered, axis=-1, keepdims=True))
    return (centered * lax.rsqrt(spread + EPS) * gain).astype(jnp.bfloat16)

def attend(qkv_rows, segment_ids, patch_mask, head_dim):
    count = qkv_rows.shape[0]
    heads = qkv_rows.shape[2] // head_dim
    split = qkv_rows.reshape(count, 3, heads, head_dim)
    query = split[:, 0].astype(jnp.float32)
    keys = split[:, 1].astype(jnp.float32)
    values = split[:, 2].astype(jnp.float32)
    scores = jnp.einsum('qhd,khd->hqk', query, keys) / math.sqrt(head_dim)
    places = jnp.arange(count)
    visible = (segment_ids[:, None] == segment_ids[None, :]) & (patch_mask[None, :] > 0) | (places[:, None] == places[None, :])
    scores = jnp.where(visible[None], scores, -1e+30)
    peak = lax.optimization_barrier(jnp.max(scores, axis=-1, keepdims=True))
    weights = jnp.exp(scores - peak)
    total = lax.optimization_barrier(jnp.sum(weights, axis=-1, keepdims=True))
    probs = (weights / total).astype(jnp.bfloat16).astype(jnp.float32)
    mixed = jnp.einsum('hqk,khd->qhd', probs, values)
    return mixed.astype(jnp.bfloat16).reshape(count, heads * head_dim)

def reference(tokens, qkv_weight, out_weight, fc1_weight, fc2_weight, norm1_gain, norm2_gain, norm3_gain, proj_weight, grid_h, grid_w, segment_ids, patch_mask, owner):
    req_count = REQUESTS // REQ_DEV
    qkv_flat = qkv_weight.reshape(D, 3 * D)

    def encode(block):
        rows, segs, masks = block
        resid = rows.astype(jnp.float32)
        normed = layer_norm(resid, norm1_gain)
        qkv_rows = jnp.dot(normed, qkv_flat, preferred_element_type=jnp.float32).astype(jnp.bfloat16).reshape(TOK_DEV, 3, D)
        mixed = attend(qkv_rows, segs, masks, HD)
        resid1 = resid + jnp.dot(mixed, out_weight, preferred_element_type=jnp.float32)
        normed2 = layer_norm(resid1, norm2_gain)
        hidden = jax.nn.gelu(jnp.dot(normed2, fc1_weight, preferred_element_type=jnp.float32), approximate=False).astype(jnp.bfloat16)
        resid2 = resid1 + jnp.dot(hidden, fc2_weight, preferred_element_type=jnp.float32)
        final = layer_norm(resid2, norm3_gain)
        merged = final.reshape(TOK_DEV // 4, 4 * D)
        return jnp.dot(merged, proj_weight, preferred_element_type=jnp.float32)
    projected = lax.map(encode, (tokens.reshape(req_count, TOK_DEV, D), segment_ids.reshape(req_count, TOK_DEV), patch_mask.reshape(req_count, TOK_DEV)))
    merged_len = (grid_h * grid_w // 4).astype(jnp.int32)
    per_dev = merged_len.reshape(req_count, REQ_DEV)
    starts = (jnp.cumsum(per_dev, axis=1) - per_dev).reshape(-1).astype(jnp.int32)
    numbers = jnp.arange(REQUESTS).astype(jnp.int32)
    source_of = numbers // REQ_DEV
    offset_of = jnp.mod(owner - source_of, req_count)
    slot_of = owner * REQ_DEV + offset_of
    match = slot_of[None, :] == numbers[:, None]
    request_of_slot = lax.optimization_barrier(jnp.sum(jnp.where(match, numbers[None, :], 0), axis=1)).astype(jnp.int32)
    source = request_of_slot // REQ_DEV
    start = starts[request_of_slot]
    count = merged_len[request_of_slot]
    steps_idx = jnp.arange(MCAP).astype(jnp.int32)
    index = jnp.minimum(start[:, None] + steps_idx[None, :], TOK_DEV // 4 - 1).astype(jnp.int32)
    rows_out = projected[source[:, None], index]
    rows_out = jnp.where((steps_idx[None, :] < count[:, None])[:, :, None], rows_out, jnp.zeros_like(rows_out))
    pooled = lax.optimization_barrier(jnp.sum(rows_out, axis=1)) / count[:, None].astype(jnp.float32)
    scale = jnp.sqrt(lax.optimization_barrier(jnp.sum(pooled * pooled, axis=1)) / OUT + EPS)
    top = lax.optimization_barrier(jnp.max(pooled, axis=1)) / scale
    return (rows_out.reshape(REQUESTS * MCAP, OUT).astype(jnp.bfloat16), scale, top)
```

```python
import functools
import math

import jax
import jax.numpy as jnp
from jax import lax
from jax.experimental import pallas as pl
from jax.experimental.pallas import tpu as pltpu
from jax.sharding import PartitionSpec as P

HD = 104
OUT = 4096


EPS = 1e-06


def shifted(value, axis, steps):
    count = lax.axis_size(axis)
    pairs = [(source, (source + steps) % count) for source in range(count)]
    return lax.ppermute(value, axis, pairs)


def layer_norm(rows, gain):
    mean = jnp.mean(rows, axis=-1, keepdims=True)
    centered = rows - mean
    spread = jnp.mean(centered * centered, axis=-1, keepdims=True)
    return (centered * lax.rsqrt(spread + EPS) * gain).astype(jnp.bfloat16)


def attend(qkv_rows, segment_ids, patch_mask, head_dim):
    count = qkv_rows.shape[0]
    heads = qkv_rows.shape[2] // head_dim
    split = qkv_rows.reshape(count, 3, heads, head_dim)
    query, keys, values = (split[:, 0], split[:, 1], split[:, 2])
    scores = jnp.einsum(
        "qhd,khd->hqk", query, keys, preferred_element_type=jnp.float32
    ) / math.sqrt(head_dim)
    places = jnp.arange(count)
    visible = (segment_ids[:, None] == segment_ids[None, :]) & (patch_mask[None, :] > 0) | (
        places[:, None] == places[None, :]
    )
    scores = jnp.where(visible[None], scores, -1e30)
    peak = jnp.max(scores, axis=-1, keepdims=True)
    weights = jnp.exp(scores - peak)
    total = jnp.sum(weights, axis=-1, keepdims=True)
    probs = (weights / total).astype(jnp.bfloat16)
    mixed = jnp.einsum("hqk,khd->qhd", probs, values, preferred_element_type=jnp.float32)
    return mixed.astype(jnp.bfloat16).reshape(count, heads * head_dim)


def shards(
    tokens,
    qkv_weight,
    out_weight,
    fc1_weight,
    fc2_weight,
    norm1_gain,
    norm2_gain,
    norm3_gain,
    proj_weight,
    grid_h,
    grid_w,
    segment_ids,
    patch_mask,
    owner,
):
    rows = tokens.shape[0]
    width = tokens.shape[1]
    share = rows // lax.axis_size("tp")
    resid = tokens.astype(jnp.float32)
    normed = layer_norm(resid, norm1_gain)
    columns = normed
    qkv_rows = jnp.einsum(
        "rd,dcj->rcj",
        columns,
        lax.all_gather(qkv_weight, "req", axis=0, tiled=True),
        preferred_element_type=jnp.float32,
    ).astype(jnp.bfloat16)
    mixed = attend(qkv_rows, segment_ids, patch_mask, HD)
    attn_part = jnp.dot(
        mixed,
        lax.all_gather(out_weight, "req", axis=1, tiled=True),
        preferred_element_type=jnp.float32,
    )
    first = lax.axis_index("tp") * share
    resid1 = lax.dynamic_slice_in_dim(resid, first, share, 0) + lax.psum_scatter(
        attn_part, "tp", scatter_dimension=0, tiled=True
    )
    normed2 = lax.all_gather(layer_norm(resid1, norm2_gain), "tp", axis=0, tiled=True)
    columns = normed2
    before = jnp.dot(
        columns,
        lax.all_gather(fc1_weight, "req", axis=0, tiled=True),
        preferred_element_type=jnp.float32,
    )
    hidden = jax.nn.gelu(before, approximate=False).astype(jnp.bfloat16)
    resid2 = resid1 + lax.psum_scatter(
        jnp.dot(
            hidden,
            lax.all_gather(fc2_weight, "req", axis=1, tiled=True),
            preferred_element_type=jnp.float32,
        ),
        "tp",
        scatter_dimension=0,
        tiled=True,
    )
    final = lax.all_gather(layer_norm(resid2, norm3_gain), "tp", axis=0, tiled=True)
    merged = final.reshape(rows // 4, 4 * width)
    req_count = lax.axis_size("req")
    here = lax.axis_index("req")
    per_dev = grid_h.shape[0] // req_count
    slots = rows // (4 * per_dev)
    merged_len = grid_h * grid_w // 4
    mine = lax.dynamic_slice_in_dim(merged_len, here * per_dev, per_dev)
    my_owner = lax.dynamic_slice_in_dim(owner, here * per_dev, per_dev)
    my_start = jnp.cumsum(mine) - mine
    offsets = jnp.mod(my_owner - here, req_count)
    pick = offsets[None, :] == jnp.arange(per_dev)[:, None]
    send_start = jnp.sum(jnp.where(pick, my_start[None, :], 0), axis=1)
    send_count = jnp.sum(jnp.where(pick, mine[None, :], 0), axis=1)
    step_index = jnp.arange(slots)
    source_of = jnp.arange(grid_h.shape[0]) // per_dev
    sources = jnp.mod(here - jnp.arange(per_dev), req_count)
    match = (owner[None, :] == here) & (source_of[None, :] == sources[:, None])
    recv_count = jnp.sum(jnp.where(match, merged_len[None, :], 0), axis=1)

    def slot_rows(table, offset):
        index = jnp.minimum(send_start[offset] + step_index, table.shape[0] - 1)
        taken = jnp.take(table, index, axis=0)
        return jnp.where((step_index < send_count[offset])[:, None], taken, jnp.zeros_like(taken))

    def project_rows(inputs):

        def add_proj(total, piece, start):
            return jnp.dot(inputs, piece, preferred_element_type=jnp.float32)

        return (add_proj, jnp.zeros((inputs.shape[0], proj_weight.shape[1]), jnp.float32))

    parcels = [slot_rows(merged, 0)]
    offset = 1
    parcels.append(shifted(slot_rows(merged, offset), "req", offset))
    owned = jnp.concatenate(parcels, axis=0)
    add_proj, proj_init = project_rows(owned)
    projected = add_proj(
        proj_init, lax.all_gather(proj_weight, "req", axis=0, tiled=True), jnp.int32(0)
    )
    blocks = projected.reshape(per_dev, slots, projected.shape[1])
    pooled = jnp.sum(blocks, axis=1) / recv_count[:, None].astype(jnp.float32)
    squares = jnp.sum(pooled * pooled, axis=1)
    largest = jnp.max(pooled, axis=1)
    total_sq = lax.psum(squares, "tp")
    peak = lax.pmax(largest, "tp")
    scale = jnp.sqrt(total_sq / OUT + EPS)
    return (projected.astype(jnp.bfloat16), scale, peak / scale)


def plain_solution(mesh):
    return jax.shard_map(
        shards,
        mesh=mesh,
        in_specs=(
            P("req", None),
            P("req", None, "tp"),
            P("tp", "req"),
            P("req", "tp"),
            P("tp", "req"),
            P(),
            P(),
            P(),
            P("req", "tp"),
            P(),
            P(),
            P("req"),
            P("req"),
            P(),
        ),
        out_specs=(P("req", "tp"), P("req"), P("req")),
        check_vma=False,
    )


def attend_group(qkv_rows, segment_ids, key_ids, head_dim):
    parts, count = segment_ids.shape
    heads = qkv_rows.shape[2] // head_dim
    split = qkv_rows.reshape(parts, count, 3, heads, head_dim)
    query, keys, values = (split[:, :, 0], split[:, :, 1], split[:, :, 2])
    scores = jnp.einsum(
        "gqhd,gkhd->ghqk", query, keys, preferred_element_type=jnp.float32
    ) / math.sqrt(head_dim)
    places = jnp.arange(count)
    visible = (segment_ids[:, :, None] == key_ids[:, None, :]) | (
        places[:, None] == places[None, :]
    )
    scores = jnp.where(visible[:, None], scores, -1e30)
    peak = jnp.max(scores, axis=-1, keepdims=True)
    weights = jnp.exp(scores - peak)
    total = jnp.sum(weights, axis=-1, keepdims=True)
    probs = (weights / total).astype(jnp.bfloat16)
    mixed = jnp.einsum("ghqk,gkhd->gqhd", probs, values, preferred_element_type=jnp.float32)
    return mixed.astype(jnp.bfloat16).reshape(parts * count, heads * head_dim)


def exchange(value, split_axis, concat_axis):
    return lax.all_to_all(value, "near", split_axis, concat_axis, tiled=True)


def ring_pairs(order):
    ahead = [(order[p], order[(p + 1) % 4]) for p in range(4)]
    return ahead, [(target, source) for source, target in ahead]


def ring_first(value, axis, order):
    if lax.axis_size(axis) != 4:
        return (value,)
    ahead, behind = ring_pairs(order)
    return value, lax.ppermute(value, axis, ahead), lax.ppermute(value, axis, behind)


def ring_second(blocks, axis, order):
    if lax.axis_size(axis) != 4:
        return lax.all_gather(blocks[0], axis, axis=0, tiled=False)
    value, left, right = blocks
    ahead, behind = ring_pairs(order)
    half = value.shape[0] // 2
    upper = lax.ppermute(left[:half], axis, ahead)
    lower = lax.ppermute(right[half:], axis, behind)
    me = lax.axis_index(axis)
    names = jnp.array(order)
    place = jnp.sum(jnp.where(names == me, jnp.arange(4), 0))

    def member(steps):
        return jnp.sum(jnp.where(jnp.arange(4) == jnp.mod(place + steps, 4), names, 0))

    out = jnp.zeros((4,) + value.shape, value.dtype)
    rest = (0,) * (value.ndim - 1)
    out = lax.dynamic_update_slice(out, value[None], (me, 0) + rest)
    out = lax.dynamic_update_slice(out, left[None], (member(3), 0) + rest)
    out = lax.dynamic_update_slice(out, right[None], (member(1), 0) + rest)
    out = lax.dynamic_update_slice(out, upper[None], (member(2), 0) + rest)
    return lax.dynamic_update_slice(out, lower[None], (member(2), half) + rest)


LINE = (0, 1, 2, 3)
PLANE = (0, 1, 3, 2)


def far_first(value):
    return ring_first(value, "far", LINE)


def far_second(blocks):
    out = ring_second(blocks, "far", LINE)
    return out.reshape((-1,) + out.shape[2:])


def gather_group(value):
    return lax.all_gather(value, ("near", "tp"), axis=0, tiled=True)


def grouped_shards(
    tokens,
    qkv_weight,
    out_weight,
    fc1_weight,
    fc2_weight,
    norm1_gain,
    norm2_gain,
    norm3_gain,
    proj_weight,
    grid_h,
    grid_w,
    segment_ids,
    patch_mask,
    owner,
):
    rows, width = tokens.shape
    near = lax.axis_size("near")
    req_count = lax.axis_size("far") * near
    group_first = lax.axis_index("far") * near
    share = rows // lax.axis_size("tp")
    first = lax.axis_index("tp") * share

    near_heads = qkv_weight.shape[2] // near
    qkv_cut = qkv_weight.reshape(-1, 3, near, near_heads).transpose(2, 0, 1, 3)
    qkv_cut = qkv_cut.reshape(near * qkv_weight.shape[0], 3 * near_heads)
    qkv, fc1_weight, fc2_weight, proj_weight, out_weight = lax.optimization_barrier(
        (exchange(qkv_cut, 0, 0), fc1_weight, fc2_weight, proj_weight, out_weight)
    )
    qkv_full = far_second(far_first(qkv))
    fc1 = exchange(fc1_weight, 1, 0)
    fc2 = exchange(fc2_weight.T, 1, 0)
    proj = exchange(proj_weight, 1, 0)

    ids = jnp.stack([segment_ids, jnp.where(patch_mask > 0, segment_ids, -1)])[None]
    ids = exchange(jnp.broadcast_to(ids, (near,) + ids.shape[1:]), 0, 0)
    resid = lax.dynamic_slice_in_dim(tokens, first, share, 0).astype(jnp.float32)
    normed = gather_group(layer_norm(resid, norm1_gain))
    normed, fc1, fc2, out_weight = lax.optimization_barrier((normed, fc1, fc2, out_weight))
    fc1 = far_first(fc1)
    out_far = ring_second(ring_first(out_weight.T, "far", LINE), "far", LINE)
    out_near = ring_first(out_far, "near", PLANE)
    qkv_rows = jnp.dot(normed, qkv_full, preferred_element_type=jnp.float32).astype(jnp.bfloat16)
    qkv_rows = qkv_rows.reshape(-1, 3, near_heads)
    mixed = attend_group(qkv_rows, ids[:, 0], ids[:, 1], HD)
    mixed, proj, out_near, fc1 = lax.optimization_barrier((mixed, proj, out_near, fc1))
    fc1_full = far_second(fc1)
    mixed = exchange(mixed, 0, 1)
    out_full = jnp.swapaxes(ring_second(out_near, "near", PLANE), 0, 1)
    out_full = out_full.reshape(width, out_weight.shape[0])
    attn_part = jnp.einsum("rk,ck->rc", mixed, out_full, preferred_element_type=jnp.float32)
    resid1 = resid + lax.psum_scatter(attn_part, "tp", scatter_dimension=0, tiled=True)
    resid1, fc1_full, fc2 = lax.optimization_barrier((resid1, fc1_full, fc2))
    fc2 = far_first(fc2)
    normed2 = gather_group(layer_norm(resid1, norm2_gain))
    normed2, proj, fc2 = lax.optimization_barrier((normed2, proj, fc2))
    fc2_full = far_second(fc2)
    proj = far_first(proj)
    before = jnp.dot(normed2, fc1_full, preferred_element_type=jnp.float32)
    hidden = jax.nn.gelu(before, approximate=False).astype(jnp.bfloat16)
    hidden, fc2_full = lax.optimization_barrier((hidden, fc2_full))
    resid2 = resid1 + lax.psum_scatter(
        jnp.einsum("rk,ck->rc", hidden, fc2_full, preferred_element_type=jnp.float32),
        ("near", "tp"),
        scatter_dimension=0,
        tiled=True,
    )
    resid2, proj = lax.optimization_barrier((resid2, proj))
    proj_full = far_second(proj)
    merged = gather_group(layer_norm(resid2, norm3_gain).reshape(share // 4, 4 * width))
    projected = jnp.dot(merged, proj_full, preferred_element_type=jnp.float32)

    per_dev = grid_h.shape[0] // req_count
    places = rows // 4
    slots = places // per_dev
    merged_len = (grid_h * grid_w // 4).reshape(req_count, per_dev)
    starts = jnp.cumsum(merged_len, axis=1) - merged_len
    offsets = jnp.mod(owner.reshape(req_count, per_dev) - jnp.arange(req_count)[:, None], req_count)
    pick = offsets[:, None, :] == jnp.arange(per_dev)[None, :, None]
    slot_start = jnp.sum(jnp.where(pick, starts[:, None, :], 0), axis=2)
    slot_count = jnp.sum(jnp.where(pick, merged_len[:, None, :], 0), axis=2)
    slot_start = lax.dynamic_slice_in_dim(slot_start, group_first, near, 0)
    slot_count = lax.dynamic_slice_in_dim(slot_count, group_first, near, 0)
    step = jnp.arange(slots)
    index = jnp.minimum(slot_start[:, :, None] + step, places - 1)
    index = index + (jnp.arange(near) * places)[:, None, None]
    taken = jnp.take(projected, index.reshape(-1), axis=0)
    live = (step < slot_count[:, :, None]).reshape(-1)
    taken = jnp.where(live[:, None], taken, jnp.zeros_like(taken))
    blocks = taken.reshape(near, per_dev, slots, taken.shape[1])
    pooled = jnp.sum(blocks, axis=2) / slot_count[:, :, None].astype(jnp.float32)
    pooled = exchange(pooled, 0, 2)[0]
    stats = jnp.stack([jnp.sum(pooled * pooled, axis=1), jnp.max(pooled, axis=1)])
    own = exchange(taken.astype(jnp.bfloat16), 0, 1)
    parcels = [own[:slots]]
    marks = [stats[:, :1]]
    for o in range(1, per_dev):
        parcels.append(shifted(own[o * slots : (o + 1) * slots], ("far", "near"), o))
        marks.append(shifted(stats[:, o : o + 1], ("far", "near"), o))
    marks = jnp.concatenate(marks, axis=1)
    scale = jnp.sqrt(lax.psum(marks[0], "tp") / OUT + EPS)
    return (jnp.concatenate(parcels, axis=0), scale, lax.pmax(marks[1], "tp") / scale)


MESH = pl.DeviceIdType.MESH
LANES = 128
NEAR = 4
FAR = 4


def padded_head(head_dim):
    return -(-head_dim // LANES) * LANES


def norm_rows(value, gain):
    mean = jnp.mean(value, axis=-1, keepdims=True)
    centered = value - mean
    spread = jnp.mean(centered * centered, axis=-1, keepdims=True)
    return (centered * lax.rsqrt(spread + EPS) * gain).astype(jnp.bfloat16)


def dot_nt(left, right):
    return lax.dot_general(left, right, (((1,), (1,)), ((), ())), preferred_element_type=jnp.float32)


def layer_kernel(
    dims,
    tok_ref,
    ids_ref,
    gain_ref,
    sel_ref,
    cnt_ref,
    qkv_in,
    out_in,
    fc1_in,
    fc2_in,
    proj_in,
    emb_ref,
    stat_ref,
    qkv_land,
    out_land,
    fc1_land,
    fc2_land,
    proj_land,
    ha,
    hb,
    w_a,
    w_b,
    w_p,
    ids_all,
    qkv_buf,
    att_buf,
    mix,
    hid,
    send,
    acc,
    core_land,
    attn_land,
    rs_land,
    resid,
    picked,
    emb_buf,
    tile_buf,
    stat_land,
    wa_s,
    wa_r,
    wl,
    b_s,
    b_r,
    c_s,
    c_r,
    o_s,
    o_r,
    h_s,
    h_r,
    k_s,
    k_r,
    i_s,
    i_r,
    m_s,
    m_r,
    ca_s,
    ca_r,
    cr_s,
    cr_r,
    rr_s,
    rr_r,
    e_s,
    e_r,
    t_s,
    t_r,
    ld,
):
    half, width, hp, heads, slots = dims
    z = lax.axis_index("far")
    q = lax.axis_index("near")
    c = lax.axis_index("tp")
    other = 1 - c
    ahead = lax.rem(z + 1, FAR)
    behind = lax.rem(z + FAR - 1, FAR)
    opposite = lax.rem(z + 2, FAR)
    rows = 2 * half
    scale = math.sqrt(HD)

    def peer(d):
        return lax.rem(q + d, NEAR)

    def source(d):
        return lax.rem(q + NEAR - d, NEAR)

    def remote(src, dst, s, r, device):
        return pltpu.make_async_remote_copy(
            src_ref=src, dst_ref=dst, send_sem=s, recv_sem=r, device_id=device, device_id_type=MESH
        )

    def rows_of(ref, first, count, step):
        return ref.at[pl.ds(pl.multiple_of(first, step), count)]

    depth = fc1_in.shape[0]
    piece = (
        lambda n: qkv_in.at[n],
        lambda n: fc1_in.at[:, pl.ds(pl.multiple_of(n * w_a.shape[1], LANES), w_a.shape[1])],
        lambda n: fc2_in.at[:, pl.ds(pl.multiple_of(n * w_b.shape[1], LANES), w_b.shape[1])],
        lambda n: proj_in.at[:, pl.ds(pl.multiple_of(n * w_p.shape[1], LANES), w_p.shape[1])],
    )
    lands = (qkv_land, fc1_land, fc2_land, proj_land)
    deep = (depth, depth, depth, proj_in.shape[0])

    def near_copy(w, d):
        dst = rows_of(lands[w], deep[w] * (NEAR * z + q), deep[w], 8)
        return remote(piece[w](peer(d)), dst, wa_s.at[w, d - 1], wa_r.at[w, d - 1], (z, peer(d), c))

    def near_own(w):
        dst = rows_of(lands[w], deep[w] * (NEAR * z + q), deep[w], 8)
        return pltpu.make_async_copy(piece[w](q), dst, wl.at[w])

    def near_start(w):
        for d in range(1, NEAR):
            near_copy(w, d).start()
        near_own(w).start()

    def near_wait(w):
        for d in range(1, NEAR):
            near_copy(w, d).wait_recv()
        near_own(w).wait()

    def far_block(w, place):
        if w == 4:
            return rows_of(out_land, depth * (NEAR * place + q), depth, 8)
        return rows_of(lands[w], NEAR * deep[w] * place, NEAR * deep[w], 16)

    def far_half(w, place, part):
        if w == 4:
            wide = out_land.shape[1] // 2
            first = pl.multiple_of(depth * (NEAR * place + q), 8)
            return out_land.at[pl.ds(first, depth), pl.ds(part * wide, wide)]
        many = NEAR * deep[w]
        return rows_of(lands[w], many * place + part * (many // 2), many // 2, 16)

    def far_b(w, way):
        src = out_in if w == 4 else far_block(w, z)
        return remote(src, far_block(w, z), b_s.at[w, way], b_r.at[w, way], ((ahead, behind)[way], q, c))

    def far_c(w, way):
        place = (behind, ahead)[way]
        part = far_half(w, place, way)
        return remote(part, part, c_s.at[w, way], c_r.at[w, way], ((ahead, behind)[way], q, c))

    def far_start(w):
        for way in (0, 1):
            far_b(w, way).start()

    def far_pass(w):
        for way in (0, 1):
            far_b(w, way).wait_recv()
            far_c(w, way).start()

    def far_wait(w):
        for way in (0, 1):
            far_c(w, way).wait_recv()

    def out_copy(k, d):
        place = (z, behind, ahead, opposite)[k]
        block = far_block(4, place)
        return remote(out_in if k == 0 else block, block, o_s.at[k, d - 1], o_r.at[k, d - 1], (z, peer(d), c))

    def out_start(k):
        for d in range(1, NEAR):
            out_copy(k, d).start()

    out_own = pltpu.make_async_copy(out_in, far_block(4, z), wl.at[4])

    def slot(p, core):
        return 2 * p + core

    def h_copy(ph, buf, d):
        block = buf.at[slot(q, c)]
        return remote(block, block, h_s.at[ph, d - 1], h_r.at[ph, d - 1], (z, peer(d), c))

    def h_core(ph, buf, d):
        block = buf.at[slot(source(d), c)]
        return remote(block, block, k_s.at[ph, d], k_r.at[ph, d], (z, q, other))

    def h_start(ph, buf):
        for d in range(1, NEAR):
            h_copy(ph, buf, d).start()
        h_core(ph, buf, 0).start()

    def h_pass(ph, buf):
        for d in range(1, NEAR):
            h_copy(ph, buf, d).wait_recv()
            h_core(ph, buf, d).start()

    def h_wait(ph, buf):
        for d in range(NEAR):
            h_core(ph, buf, d).wait_recv()

    def h_done(ph, buf):
        for d in range(1, NEAR):
            h_copy(ph, buf, d).wait_send()
        for d in range(NEAR):
            h_core(ph, buf, d).wait_send()

    def ids_copy(d):
        return remote(ids_ref, ids_all.at[q], i_s.at[d - 1], i_r.at[d - 1], (z, peer(d), c))

    near_start(0)
    far_start(4)
    out_start(0)
    out_own.start()
    for d in range(1, NEAR):
        ids_copy(d).start()
    ids_all[q] = ids_ref[...]

    step = 64
    mine = slot(q, c)

    def first_norm(t, _):
        at = pl.ds(pl.multiple_of(t * step, step), step)
        value = tok_ref[at, :].astype(jnp.float32)
        ha[mine, at, :] = norm_rows(value, gain_ref[0:1, :])
        return 0

    lax.fori_loop(0, half // step, first_norm, 0)
    h_start(0, ha)
    near_wait(0)
    far_start(0)
    near_start(1)
    h_pass(0, ha)
    near_start(2)
    near_start(3)

    for way in (0, 1):
        far_b(4, way).wait_recv()
        far_c(4, way).start()
        out_start(1 + way)
    far_pass(0)
    near_wait(1)
    far_start(1)
    far_wait(4)
    out_start(3)
    h_wait(0, ha)
    for d in range(1, NEAR):
        ids_copy(d).wait_recv()
    far_wait(0)

    load_q = pltpu.make_async_copy(qkv_land, w_a.at[:, pl.ds(0, qkv_land.shape[1])], ld.at[0])
    load_q.start()
    load_q.wait()
    triple = qkv_land.shape[1]

    def qkv_rows(s, _):
        got = ha[s]
        for n in range(triple // 256):
            part = jnp.dot(got, w_a[:, n * 256 : (n + 1) * 256], preferred_element_type=jnp.float32)
            qkv_buf[s, :, n * 256 : (n + 1) * 256] = part.astype(jnp.bfloat16)
        return 0

    lax.fori_loop(0, 2 * NEAR, qkv_rows, 0)

    group = heads * hp

    def mix_copy(d):
        lanes = pl.ds(pl.multiple_of(q * group, LANES), group)
        return remote(
            att_buf.at[peer(d)], mix.at[:, lanes], m_s.at[d - 1], m_r.at[d - 1], (z, peer(d), c)
        )

    def attend_rows(p, h, t):
        query = qkv_buf[2 * p + t, :, h * hp : (h + 1) * hp]
        keys = qkv_buf[pl.ds(2 * p, 2), :, group + h * hp : group + (h + 1) * hp]
        values = qkv_buf[pl.ds(2 * p, 2), :, 2 * group + h * hp : 2 * group + (h + 1) * hp]
        scores = dot_nt(query, keys.reshape(rows, hp)) / scale
        segment = jnp.transpose(ids_all[p, :, t * half : (t + 1) * half])[:, 0:1]
        key_ids = ids_all[p, 1:2, :]
        place = lax.broadcasted_iota(jnp.int32, (half, rows), 0) + t * half
        column = lax.broadcasted_iota(jnp.int32, (half, rows), 1)
        visible = (segment == key_ids) | (place == column)
        scores = jnp.where(visible, scores, -1e30)
        peak = jnp.max(scores, axis=-1, keepdims=True)
        weights = jnp.exp(scores - peak)
        total = jnp.sum(weights, axis=-1, keepdims=True)
        probs = (weights / total).astype(jnp.bfloat16)
        mixed = jnp.dot(probs, values.reshape(rows, hp), preferred_element_type=jnp.float32)
        att_buf[p, t * half : (t + 1) * half, h * hp : (h + 1) * hp] = mixed.astype(jnp.bfloat16)

    for d in (1, 2, 3, 0):
        target = peer(d)
        for h in range(heads):
            for t in range(2):
                attend_rows(target, h, t)
        if d:
            mix_copy(d).start()
    mix[:, pl.ds(pl.multiple_of(q * group, LANES), group)] = att_buf[q]

    for k in range(4):
        for d in range(1, NEAR):
            out_copy(k, d).wait_recv()
    out_own.wait()
    load_o = pltpu.make_async_copy(out_land, w_b, ld.at[1])
    load_o.start()
    load_o.wait()
    for d in range(1, NEAR):
        mix_copy(d).wait_recv()

    tile = 128
    tiles = width // tile

    def attn_copy():
        return remote(send.at[0], attn_land, ca_s.at[0], ca_r.at[0], (z, q, other))

    def out_rows(dst, core):
        got = mix[pl.ds(pl.multiple_of(core * half, 16), half), :]
        for n in range(tiles):
            dst[:, n * tile : (n + 1) * tile] = dot_nt(got, w_b[n * tile : (n + 1) * tile, :])

    out_rows(send.at[0], other)
    attn_copy().start()
    out_rows(resid, c)
    h_done(0, ha)
    attn_copy().wait_recv()

    def second_norm(t, _):
        at = pl.ds(pl.multiple_of(t * step, step), step)
        value = tok_ref[at, :].astype(jnp.float32) + (resid[at, :] + attn_land[at, :])
        resid[at, :] = value
        hb[mine, at, :] = norm_rows(value, gain_ref[1:2, :])
        return 0

    lax.fori_loop(0, half // step, second_norm, 0)
    h_start(1, hb)
    far_pass(1)
    near_wait(2)
    far_start(2)
    h_pass(1, hb)
    far_wait(1)
    load_1 = pltpu.make_async_copy(fc1_land, w_a, ld.at[2])
    load_1.start()
    load_1.wait()
    h_wait(1, hb)
    hidden = w_a.shape[1]

    def fc1_rows(s, _):
        got = hb[s]
        for n in range(hidden // 256):
            part = jnp.dot(got, w_a[:, n * 256 : (n + 1) * 256], preferred_element_type=jnp.float32)
            part = 0.5 * part * (1.0 + lax.erf(part * math.sqrt(0.5)))
            hid[s, :, n * 256 : (n + 1) * 256] = part.astype(jnp.bfloat16)
        return 0

    lax.fori_loop(0, 2 * NEAR, fc1_rows, 0)
    h_done(1, hb)
    attn_copy().wait_send()

    far_pass(2)
    near_wait(3)
    far_start(3)
    far_wait(2)
    load_2 = pltpu.make_async_copy(fc2_land, w_b, ld.at[3])
    load_2.start()
    load_2.wait()

    def fc2_rows(dst, s):
        got = hid[s]
        for n in range(tiles):
            dst[:, n * tile : (n + 1) * tile] = dot_nt(got, w_b[n * tile : (n + 1) * tile, :])

    order = (1, 2, 3, 0)

    def core_copy(i):
        return remote(send.at[i % 2], core_land.at[i], cr_s.at[i], cr_r.at[i], (z, q, other))

    def rs_copy(d):
        return remote(acc.at[d], rs_land.at[d - 1], rr_s.at[d - 1], rr_r.at[d - 1], (z, peer(d), c))

    def join(i):
        d = order[i]
        core_copy(i).wait_recv()

        def add(t, _):
            at = pl.ds(pl.multiple_of(t * step, step), step)
            acc[d, at, :] = acc[d, at, :] + core_land[i, at, :]
            return 0

        lax.fori_loop(0, half // step, add, 0)
        if d:
            rs_copy(d).start()

    for i in range(4):
        target = peer(order[i])
        if i >= 2:
            core_copy(i - 2).wait_send()
        fc2_rows(send.at[i % 2], slot(target, other))
        core_copy(i).start()
        fc2_rows(acc.at[order[i]], slot(target, c))
        join(i)

    for d in range(1, NEAR):
        rs_copy(d).wait_recv()

    def third_norm(t, _):
        at = pl.ds(pl.multiple_of(t * step, step), step)
        value = resid[at, :] + ((acc[0, at, :] + rs_land[0, at, :]) + (rs_land[1, at, :] + rs_land[2, at, :]))
        picked[at, :] = norm_rows(value, gain_ref[2:3, :])
        return 0

    lax.fori_loop(0, half // step, third_norm, 0)
    quarter = half // 2
    for j in range(2):
        got = jnp.dot(
            sel_ref[...], picked[j * quarter : (j + 1) * quarter, :], preferred_element_type=jnp.float32
        )
        ha[mine, j * quarter : (j + 1) * quarter, :] = got.astype(jnp.bfloat16)
    h_start(2, ha)
    far_pass(3)
    h_pass(2, ha)
    far_wait(3)
    load_p = pltpu.make_async_copy(proj_land, w_p, ld.at[4])
    load_p.start()
    load_p.wait()
    h_wait(2, ha)

    wide = w_p.shape[1]
    cols = pl.ds(pl.multiple_of(q * wide, LANES), wide)

    def emb_copy(o, d):
        at = pl.ds(o * slots, slots)
        if o == 0:
            device = (z, peer(d), c)
            src = emb_buf.at[peer(d), at]
        else:
            owner = peer(d)
            step_z = 1 - jnp.minimum(owner, 1)
            device = (lax.rem(z + step_z, FAR), owner, c)
            src = emb_buf.at[lax.rem(owner + NEAR - 1, NEAR), at]
        return remote(src, emb_ref.at[at, cols], e_s.at[o, d], e_r.at[o, d], device)

    def emb_own(o):
        at = pl.ds(o * slots, slots)
        src = emb_buf.at[q if o == 0 else lax.rem(q + NEAR - 1, NEAR), at]
        return pltpu.make_async_copy(src, emb_ref.at[at, cols], wl.at[5 + o])

    def stat_copy(o, d, k):
        owner = peer(d)
        core = c if k == 0 else other
        if o == 0:
            device = (z, owner, core)
            src = tile_buf.at[owner, 0]
        else:
            step_z = 1 - jnp.minimum(owner, 1)
            device = (lax.rem(z + step_z, FAR), owner, core)
            src = tile_buf.at[lax.rem(owner + NEAR - 1, NEAR), 1]
        return remote(src, stat_land.at[o, mine], t_s.at[o, d, k], t_r.at[o, d, k], device)

    def proj_rows(p, _):
        total = jnp.zeros((quarter, wide), jnp.float32)
        for core in range(2):
            for j in range(2):
                got = ha[2 * p + core, j * quarter : (j + 1) * quarter, :]
                first = (2 * core + j) * width
                total = total + jnp.dot(got, w_p[first : first + width, :], preferred_element_type=jnp.float32)
        emb_buf[p] = total.astype(jnp.bfloat16)
        for o in range(2):
            pooled = jnp.sum(total[o * slots : (o + 1) * slots], axis=0, keepdims=True) / cnt_ref[
                pl.ds(2 * p + o, 1), 0:1
            ]
            squares = jnp.sum(pooled * pooled, axis=1, keepdims=True)
            largest = jnp.max(pooled, axis=1, keepdims=True)
            line = lax.broadcasted_iota(jnp.int32, (8, LANES), 0)
            tile_buf[p, o] = jnp.where(line == 0, squares, largest)
        return 0

    lax.fori_loop(0, NEAR, proj_rows, 0)

    for d in range(1, NEAR):
        for o in range(2):
            emb_copy(o, d).start()
            for k in range(2):
                stat_copy(o, d, k).start()
    emb_own(0).start()
    stat_land[0, mine] = tile_buf[q, 0]
    stat_copy(0, 0, 1).start()
    stat_copy(1, 0, 1).start()

    @pl.when(q == 0)
    def _():
        emb_copy(1, 0).start()
        stat_copy(1, 0, 0).start()

    @pl.when(q != 0)
    def _():
        emb_own(1).start()
        stat_land[1, mine] = tile_buf[lax.rem(q + NEAR - 1, NEAR), 1]
        emb_own(1).wait()

    emb_own(0).wait()
    for d in range(1, NEAR):
        for o in range(2):
            emb_copy(o, d).wait()
            for k in range(2):
                stat_copy(o, d, k).wait()
    stat_copy(0, 0, 1).wait()
    stat_copy(1, 0, 1).wait()

    @pl.when(q == 0)
    def _():
        emb_copy(1, 0).wait()
        stat_copy(1, 0, 0).wait()

    line = lax.broadcasted_iota(jnp.int32, (8, LANES), 0)
    result = jnp.zeros((8, LANES), jnp.float32)
    features = wide * NEAR * 2
    for o in range(2):
        squares = jnp.zeros((1, LANES), jnp.float32)
        largest = stat_land[o, 0, 1:2, :]
        for s in range(2 * NEAR):
            squares = squares + stat_land[o, s, 0:1, :]
            largest = jnp.maximum(largest, stat_land[o, s, 1:2, :])
        norm = jnp.sqrt(squares / features + EPS)
        result = jnp.where(line == 2 * o, norm, result)
        result = jnp.where(line == 2 * o + 1, largest / norm, result)
    stat_ref[...] = result

    for w in range(4):
        for d in range(1, NEAR):
            near_copy(w, d).wait_send()
    for w in range(5):
        for way in (0, 1):
            far_b(w, way).wait_send()
            far_c(w, way).wait_send()
    for k in range(4):
        for d in range(1, NEAR):
            out_copy(k, d).wait_send()
    for d in range(1, NEAR):
        ids_copy(d).wait_send()
        mix_copy(d).wait_send()
        rs_copy(d).wait_send()
    for i in (2, 3):
        core_copy(i).wait_send()
    h_done(2, ha)


def kernel_shards(
    tokens,
    qkv_weight,
    out_weight,
    fc1_weight,
    fc2_weight,
    norm1_gain,
    norm2_gain,
    norm3_gain,
    proj_weight,
    grid_h,
    grid_w,
    segment_ids,
    patch_mask,
    owner,
):
    rows, width = tokens.shape
    here = lax.axis_index("far") * NEAR + lax.axis_index("near")
    core = lax.axis_index("tp")
    half = rows // 2
    places = rows // 4
    hp = padded_head(HD)
    depth = qkv_weight.shape[0]
    all_heads = qkv_weight.shape[2] // HD
    heads = all_heads // NEAR

    tok = lax.dynamic_slice_in_dim(tokens.reshape(places, 4, width), 2 * core, 2, 1)
    tok = tok.transpose(1, 0, 2).reshape(half, width)
    ids = jnp.stack([segment_ids, jnp.where(patch_mask > 0, segment_ids, -1)])
    ids = ids.reshape(2, places, 4).transpose(0, 2, 1).reshape(2, rows).astype(jnp.float32)
    ids = jnp.pad(ids, ((0, 6), (0, 0)))
    gains = jnp.pad(jnp.stack([norm1_gain, norm2_gain, norm3_gain]), ((0, 5), (0, 0)))

    per_dev = 2
    slots = places // per_dev
    req_count = NEAR * FAR
    merged_len = (grid_h * grid_w // 4).reshape(req_count, per_dev)
    starts = jnp.cumsum(merged_len, axis=1) - merged_len
    offsets = jnp.mod(owner.reshape(req_count, per_dev) - jnp.arange(req_count)[:, None], req_count)
    pick = offsets[:, None, :] == jnp.arange(per_dev)[None, :, None]
    slot_start = jnp.sum(jnp.where(pick, starts[:, None, :], 0), axis=2)
    slot_count = jnp.sum(jnp.where(pick, merged_len[:, None, :], 0), axis=2)
    my_start = lax.dynamic_slice_in_dim(slot_start, here, 1, 0).reshape(per_dev, 1, 1)
    my_count = lax.dynamic_slice_in_dim(slot_count, here, 1, 0).reshape(per_dev, 1, 1)
    step = jnp.arange(slots).reshape(1, slots, 1)
    place = jnp.arange(places).reshape(1, 1, places)
    sel = (place == my_start + step) & (step < my_count)
    sel = sel.reshape(places, places).astype(jnp.bfloat16)
    counts = lax.dynamic_slice_in_dim(slot_count, lax.axis_index("far") * NEAR, NEAR, 0)
    counts = jnp.broadcast_to(counts.reshape(2 * NEAR, 1).astype(jnp.float32), (2 * NEAR, LANES))

    extra = ((0, 0),) * 4 + ((0, hp - HD),)
    cut = jnp.pad(qkv_weight.reshape(depth, 3, NEAR, heads, HD), extra)
    cut = cut.transpose(2, 0, 1, 3, 4).reshape(NEAR, depth, 3 * heads * hp)
    out_t = jnp.pad(out_weight.T.reshape(depth, all_heads, HD), extra[:2] + extra[-1:])
    out_t = out_t.reshape(depth, all_heads * hp)
    fc2_t = fc2_weight.T

    hidden = fc1_weight.shape[1] // NEAR
    wide = proj_weight.shape[1] // NEAR
    bf16, f32 = jnp.bfloat16, jnp.float32
    shape = jax.ShapeDtypeStruct
    vmem = pl.BlockSpec(memory_space=pltpu.VMEM)
    anyw = pl.BlockSpec(memory_space=pl.ANY)
    dma = pltpu.SemaphoreType.DMA
    outs = pl.pallas_call(
        functools.partial(layer_kernel, (half, width, hp, heads, slots)),
        out_shape=(
            shape((places, proj_weight.shape[1]), bf16),
            shape((8, LANES), f32),
            shape((width, cut.shape[2]), bf16),
            shape((width, out_t.shape[1]), bf16),
            shape((width, hidden), bf16),
            shape((width, hidden), bf16),
            shape((4 * width, wide), bf16),
        ),
        in_specs=[vmem] * 5 + [anyw] * 5,
        out_specs=(anyw, vmem) + (anyw,) * 5,
        scratch_shapes=[
            pltpu.VMEM((2 * NEAR, half, width), bf16),
            pltpu.VMEM((2 * NEAR, half, width), bf16),
            pltpu.VMEM((width, hidden), bf16),
            pltpu.VMEM((width, hidden), bf16),
            pltpu.VMEM((4 * width, wide), bf16),
            pltpu.VMEM((NEAR, 8, rows), f32),
            pltpu.VMEM((2 * NEAR, half, cut.shape[2]), bf16),
            pltpu.VMEM((NEAR, rows, heads * hp), bf16),
            pltpu.VMEM((rows, all_heads * hp), bf16),
            pltpu.VMEM((2 * NEAR, half, hidden), bf16),
            pltpu.VMEM((2, half, width), f32),
            pltpu.VMEM((NEAR, half, width), f32),
            pltpu.VMEM((NEAR, half, width), f32),
            pltpu.VMEM((half, width), f32),
            pltpu.VMEM((NEAR - 1, half, width), f32),
            pltpu.VMEM((half, width), f32),
            pltpu.VMEM((half, width), bf16),
            pltpu.VMEM((NEAR, places, wide), bf16),
            pltpu.VMEM((NEAR, 2, 8, LANES), f32),
            pltpu.VMEM((2, 2 * NEAR, 8, LANES), f32),
            dma((4, 3)),
            dma((4, 3)),
            dma((7,)),
            dma((5, 2)),
            dma((5, 2)),
            dma((5, 2)),
            dma((5, 2)),
            dma((4, 3)),
            dma((4, 3)),
            dma((3, 3)),
            dma((3, 3)),
            dma((3, 4)),
            dma((3, 4)),
            dma((3,)),
            dma((3,)),
            dma((3,)),
            dma((3,)),
            dma((1,)),
            dma((1,)),
            dma((4,)),
            dma((4,)),
            dma((3,)),
            dma((3,)),
            dma((2, 4)),
            dma((2, 4)),
            dma((2, 4, 2)),
            dma((2, 4, 2)),
            dma((5,)),
        ],
        compiler_params=pltpu.CompilerParams(vmem_limit_bytes=67043328, has_side_effects=True),
        name="layer",
    )(tok, ids, gains, sel, counts, cut, out_t, fc1_weight, fc2_t, proj_weight)
    stats = outs[1]
    norms = jnp.stack([stats[0, 0], stats[2, 0]])
    tops = jnp.stack([stats[1, 0], stats[3, 0]])
    return outs[0], norms, tops


def group_of(mesh, args):
    tp, req = mesh.shape["tp"], mesh.shape["req"]
    for near in (4, 2):
        whole = req % near == 0
        heads = args[1].shape[2] // (HD * tp)
        if whole and heads % near == 0:
            return near
    return 1


def solution(mesh):
    def step(*args):
        near = group_of(mesh, args)
        if near == 1:
            return plain_solution(mesh)(*args)
        tp, req = mesh.shape["tp"], mesh.shape["req"]
        split = jax.sharding.Mesh(
            mesh.devices.reshape(req // near, near, tp), ("far", "near", "tp")
        )
        both = ("far", "near")
        whole = tp == 2 and near == NEAR and req == NEAR * FAR and args[9].shape[0] == 2 * req
        return jax.shard_map(
            kernel_shards if whole else grouped_shards,
            mesh=split,
            in_specs=(
                P(both, None),
                P(both, None, "tp"),
                P("tp", both),
                P(both, "tp"),
                P("tp", both),
                P(),
                P(),
                P(),
                P(both, "tp"),
                P(),
                P(),
                P(both),
                P(both),
                P(),
            ),
            out_specs=(P(both, "tp"), P(both), P(both)),
            check_vma=False,
        )(*args)

    return step
```

```python
import functools
import math

import jax
import jax.numpy as jnp
from jax import lax
from jax.experimental import pallas as pl
from jax.experimental.pallas import tpu as pltpu
from jax.sharding import PartitionSpec as P

HD = 104
OUT = 4096


EPS = 1e-06


def shifted(value, axis, steps):
    count = lax.axis_size(axis)
    pairs = [(source, (source + steps) % count) for source in range(count)]
    return lax.ppermute(value, axis, pairs)


def layer_norm(rows, gain):
    mean = jnp.mean(rows, axis=-1, keepdims=True)
    centered = rows - mean
    spread = jnp.mean(centered * centered, axis=-1, keepdims=True)
    return (centered * lax.rsqrt(spread + EPS) * gain).astype(jnp.bfloat16)


def attend(qkv_rows, segment_ids, patch_mask, head_dim):
    count = qkv_rows.shape[0]
    heads = qkv_rows.shape[2] // head_dim
    split = qkv_rows.reshape(count, 3, heads, head_dim)
    query, keys, values = (split[:, 0], split[:, 1], split[:, 2])
    scores = jnp.einsum(
        "qhd,khd->hqk", query, keys, preferred_element_type=jnp.float32
    ) / math.sqrt(head_dim)
    places = jnp.arange(count)
    visible = (segment_ids[:, None] == segment_ids[None, :]) & (patch_mask[None, :] > 0) | (
        places[:, None] == places[None, :]
    )
    scores = jnp.where(visible[None], scores, -1e30)
    peak = jnp.max(scores, axis=-1, keepdims=True)
    weights = jnp.exp(scores - peak)
    total = jnp.sum(weights, axis=-1, keepdims=True)
    probs = (weights / total).astype(jnp.bfloat16)
    mixed = jnp.einsum("hqk,khd->qhd", probs, values, preferred_element_type=jnp.float32)
    return mixed.astype(jnp.bfloat16).reshape(count, heads * head_dim)


def shards(
    tokens,
    qkv_weight,
    out_weight,
    fc1_weight,
    fc2_weight,
    norm1_gain,
    norm2_gain,
    norm3_gain,
    proj_weight,
    grid_h,
    grid_w,
    segment_ids,
    patch_mask,
    owner,
):
    rows = tokens.shape[0]
    width = tokens.shape[1]
    share = rows // lax.axis_size("tp")
    resid = tokens.astype(jnp.float32)
    normed = layer_norm(resid, norm1_gain)
    columns = normed
    qkv_rows = jnp.einsum(
        "rd,dcj->rcj",
        columns,
        lax.all_gather(qkv_weight, "req", axis=0, tiled=True),
        preferred_element_type=jnp.float32,
    ).astype(jnp.bfloat16)
    mixed = attend(qkv_rows, segment_ids, patch_mask, HD)
    attn_part = jnp.dot(
        mixed,
        lax.all_gather(out_weight, "req", axis=1, tiled=True),
        preferred_element_type=jnp.float32,
    )
    first = lax.axis_index("tp") * share
    resid1 = lax.dynamic_slice_in_dim(resid, first, share, 0) + lax.psum_scatter(
        attn_part, "tp", scatter_dimension=0, tiled=True
    )
    normed2 = lax.all_gather(layer_norm(resid1, norm2_gain), "tp", axis=0, tiled=True)
    columns = normed2
    before = jnp.dot(
        columns,
        lax.all_gather(fc1_weight, "req", axis=0, tiled=True),
        preferred_element_type=jnp.float32,
    )
    hidden = jax.nn.gelu(before, approximate=False).astype(jnp.bfloat16)
    resid2 = resid1 + lax.psum_scatter(
        jnp.dot(
            hidden,
            lax.all_gather(fc2_weight, "req", axis=1, tiled=True),
            preferred_element_type=jnp.float32,
        ),
        "tp",
        scatter_dimension=0,
        tiled=True,
    )
    final = lax.all_gather(layer_norm(resid2, norm3_gain), "tp", axis=0, tiled=True)
    merged = final.reshape(rows // 4, 4 * width)
    req_count = lax.axis_size("req")
    here = lax.axis_index("req")
    per_dev = grid_h.shape[0] // req_count
    slots = rows // (4 * per_dev)
    merged_len = grid_h * grid_w // 4
    mine = lax.dynamic_slice_in_dim(merged_len, here * per_dev, per_dev)
    my_owner = lax.dynamic_slice_in_dim(owner, here * per_dev, per_dev)
    my_start = jnp.cumsum(mine) - mine
    offsets = jnp.mod(my_owner - here, req_count)
    pick = offsets[None, :] == jnp.arange(per_dev)[:, None]
    send_start = jnp.sum(jnp.where(pick, my_start[None, :], 0), axis=1)
    send_count = jnp.sum(jnp.where(pick, mine[None, :], 0), axis=1)
    step_index = jnp.arange(slots)
    source_of = jnp.arange(grid_h.shape[0]) // per_dev
    sources = jnp.mod(here - jnp.arange(per_dev), req_count)
    match = (owner[None, :] == here) & (source_of[None, :] == sources[:, None])
    recv_count = jnp.sum(jnp.where(match, merged_len[None, :], 0), axis=1)

    def slot_rows(table, offset):
        index = jnp.minimum(send_start[offset] + step_index, table.shape[0] - 1)
        taken = jnp.take(table, index, axis=0)
        return jnp.where((step_index < send_count[offset])[:, None], taken, jnp.zeros_like(taken))

    def project_rows(inputs):

        def add_proj(total, piece, start):
            return jnp.dot(inputs, piece, preferred_element_type=jnp.float32)

        return (add_proj, jnp.zeros((inputs.shape[0], proj_weight.shape[1]), jnp.float32))

    parcels = [slot_rows(merged, 0)]
    offset = 1
    parcels.append(shifted(slot_rows(merged, offset), "req", offset))
    owned = jnp.concatenate(parcels, axis=0)
    add_proj, proj_init = project_rows(owned)
    projected = add_proj(
        proj_init, lax.all_gather(proj_weight, "req", axis=0, tiled=True), jnp.int32(0)
    )
    blocks = projected.reshape(per_dev, slots, projected.shape[1])
    pooled = jnp.sum(blocks, axis=1) / recv_count[:, None].astype(jnp.float32)
    squares = jnp.sum(pooled * pooled, axis=1)
    largest = jnp.max(pooled, axis=1)
    total_sq = lax.psum(squares, "tp")
    peak = lax.pmax(largest, "tp")
    scale = jnp.sqrt(total_sq / OUT + EPS)
    return (projected.astype(jnp.bfloat16), scale, peak / scale)


def plain_solution(mesh):
    return jax.shard_map(
        shards,
        mesh=mesh,
        in_specs=(
            P("req", None),
            P("req", None, "tp"),
            P("tp", "req"),
            P("req", "tp"),
            P("tp", "req"),
            P(),
            P(),
            P(),
            P("req", "tp"),
            P(),
            P(),
            P("req"),
            P("req"),
            P(),
        ),
        out_specs=(P("req", "tp"), P("req"), P("req")),
        check_vma=False,
    )


def attend_group(qkv_rows, segment_ids, key_ids, head_dim):
    parts, count = segment_ids.shape
    heads = qkv_rows.shape[2] // head_dim
    split = qkv_rows.reshape(parts, count, 3, heads, head_dim)
    query, keys, values = (split[:, :, 0], split[:, :, 1], split[:, :, 2])
    scores = jnp.einsum(
        "gqhd,gkhd->ghqk", query, keys, preferred_element_type=jnp.float32
    ) / math.sqrt(head_dim)
    places = jnp.arange(count)
    visible = (segment_ids[:, :, None] == key_ids[:, None, :]) | (
        places[:, None] == places[None, :]
    )
    scores = jnp.where(visible[:, None], scores, -1e30)
    peak = jnp.max(scores, axis=-1, keepdims=True)
    weights = jnp.exp(scores - peak)
    total = jnp.sum(weights, axis=-1, keepdims=True)
    probs = (weights / total).astype(jnp.bfloat16)
    mixed = jnp.einsum("ghqk,gkhd->gqhd", probs, values, preferred_element_type=jnp.float32)
    return mixed.astype(jnp.bfloat16).reshape(parts * count, heads * head_dim)


def exchange(value, split_axis, concat_axis):
    return lax.all_to_all(value, "near", split_axis, concat_axis, tiled=True)


def ring_pairs(order):
    ahead = [(order[p], order[(p + 1) % 4]) for p in range(4)]
    return ahead, [(target, source) for source, target in ahead]


def ring_first(value, axis, order):
    if lax.axis_size(axis) != 4:
        return (value,)
    ahead, behind = ring_pairs(order)
    return value, lax.ppermute(value, axis, ahead), lax.ppermute(value, axis, behind)


def ring_second(blocks, axis, order):
    if lax.axis_size(axis) != 4:
        return lax.all_gather(blocks[0], axis, axis=0, tiled=False)
    value, left, right = blocks
    ahead, behind = ring_pairs(order)
    half = value.shape[0] // 2
    upper = lax.ppermute(left[:half], axis, ahead)
    lower = lax.ppermute(right[half:], axis, behind)
    me = lax.axis_index(axis)
    names = jnp.array(order)
    place = jnp.sum(jnp.where(names == me, jnp.arange(4), 0))

    def member(steps):
        return jnp.sum(jnp.where(jnp.arange(4) == jnp.mod(place + steps, 4), names, 0))

    out = jnp.zeros((4,) + value.shape, value.dtype)
    rest = (0,) * (value.ndim - 1)
    out = lax.dynamic_update_slice(out, value[None], (me, 0) + rest)
    out = lax.dynamic_update_slice(out, left[None], (member(3), 0) + rest)
    out = lax.dynamic_update_slice(out, right[None], (member(1), 0) + rest)
    out = lax.dynamic_update_slice(out, upper[None], (member(2), 0) + rest)
    return lax.dynamic_update_slice(out, lower[None], (member(2), half) + rest)


LINE = (0, 1, 2, 3)
PLANE = (0, 1, 3, 2)


def far_first(value):
    return ring_first(value, "far", LINE)


def far_second(blocks):
    out = ring_second(blocks, "far", LINE)
    return out.reshape((-1,) + out.shape[2:])


def gather_group(value):
    return lax.all_gather(value, ("near", "tp"), axis=0, tiled=True)


def grouped_shards(
    tokens,
    qkv_weight,
    out_weight,
    fc1_weight,
    fc2_weight,
    norm1_gain,
    norm2_gain,
    norm3_gain,
    proj_weight,
    grid_h,
    grid_w,
    segment_ids,
    patch_mask,
    owner,
):
    rows, width = tokens.shape
    near = lax.axis_size("near")
    req_count = lax.axis_size("far") * near
    group_first = lax.axis_index("far") * near
    share = rows // lax.axis_size("tp")
    first = lax.axis_index("tp") * share

    near_heads = qkv_weight.shape[2] // near
    qkv_cut = qkv_weight.reshape(-1, 3, near, near_heads).transpose(2, 0, 1, 3)
    qkv_cut = qkv_cut.reshape(near * qkv_weight.shape[0], 3 * near_heads)
    qkv, fc1_weight, fc2_weight, proj_weight, out_weight = lax.optimization_barrier(
        (exchange(qkv_cut, 0, 0), fc1_weight, fc2_weight, proj_weight, out_weight)
    )
    qkv_full = far_second(far_first(qkv))
    fc1 = exchange(fc1_weight, 1, 0)
    fc2 = exchange(fc2_weight.T, 1, 0)
    proj = exchange(proj_weight, 1, 0)

    ids = jnp.stack([segment_ids, jnp.where(patch_mask > 0, segment_ids, -1)])[None]
    ids = exchange(jnp.broadcast_to(ids, (near,) + ids.shape[1:]), 0, 0)
    resid = lax.dynamic_slice_in_dim(tokens, first, share, 0).astype(jnp.float32)
    normed = gather_group(layer_norm(resid, norm1_gain))
    normed, fc1, fc2, out_weight = lax.optimization_barrier((normed, fc1, fc2, out_weight))
    fc1 = far_first(fc1)
    out_far = ring_second(ring_first(out_weight.T, "far", LINE), "far", LINE)
    out_near = ring_first(out_far, "near", PLANE)
    qkv_rows = jnp.dot(normed, qkv_full, preferred_element_type=jnp.float32).astype(jnp.bfloat16)
    qkv_rows = qkv_rows.reshape(-1, 3, near_heads)
    mixed = attend_group(qkv_rows, ids[:, 0], ids[:, 1], HD)
    mixed, proj, out_near, fc1 = lax.optimization_barrier((mixed, proj, out_near, fc1))
    fc1_full = far_second(fc1)
    mixed = exchange(mixed, 0, 1)
    out_full = jnp.swapaxes(ring_second(out_near, "near", PLANE), 0, 1)
    out_full = out_full.reshape(width, out_weight.shape[0])
    attn_part = jnp.einsum("rk,ck->rc", mixed, out_full, preferred_element_type=jnp.float32)
    resid1 = resid + lax.psum_scatter(attn_part, "tp", scatter_dimension=0, tiled=True)
    resid1, fc1_full, fc2 = lax.optimization_barrier((resid1, fc1_full, fc2))
    fc2 = far_first(fc2)
    normed2 = gather_group(layer_norm(resid1, norm2_gain))
    normed2, proj, fc2 = lax.optimization_barrier((normed2, proj, fc2))
    fc2_full = far_second(fc2)
    proj = far_first(proj)
    before = jnp.dot(normed2, fc1_full, preferred_element_type=jnp.float32)
    hidden = jax.nn.gelu(before, approximate=False).astype(jnp.bfloat16)
    hidden, fc2_full = lax.optimization_barrier((hidden, fc2_full))
    resid2 = resid1 + lax.psum_scatter(
        jnp.einsum("rk,ck->rc", hidden, fc2_full, preferred_element_type=jnp.float32),
        ("near", "tp"),
        scatter_dimension=0,
        tiled=True,
    )
    resid2, proj = lax.optimization_barrier((resid2, proj))
    proj_full = far_second(proj)
    merged = gather_group(layer_norm(resid2, norm3_gain).reshape(share // 4, 4 * width))
    projected = jnp.dot(merged, proj_full, preferred_element_type=jnp.float32)

    per_dev = grid_h.shape[0] // req_count
    places = rows // 4
    slots = places // per_dev
    merged_len = (grid_h * grid_w // 4).reshape(req_count, per_dev)
    starts = jnp.cumsum(merged_len, axis=1) - merged_len
    offsets = jnp.mod(owner.reshape(req_count, per_dev) - jnp.arange(req_count)[:, None], req_count)
    pick = offsets[:, None, :] == jnp.arange(per_dev)[None, :, None]
    slot_start = jnp.sum(jnp.where(pick, starts[:, None, :], 0), axis=2)
    slot_count = jnp.sum(jnp.where(pick, merged_len[:, None, :], 0), axis=2)
    slot_start = lax.dynamic_slice_in_dim(slot_start, group_first, near, 0)
    slot_count = lax.dynamic_slice_in_dim(slot_count, group_first, near, 0)
    step = jnp.arange(slots)
    index = jnp.minimum(slot_start[:, :, None] + step, places - 1)
    index = index + (jnp.arange(near) * places)[:, None, None]
    taken = jnp.take(projected, index.reshape(-1), axis=0)
    live = (step < slot_count[:, :, None]).reshape(-1)
    taken = jnp.where(live[:, None], taken, jnp.zeros_like(taken))
    blocks = taken.reshape(near, per_dev, slots, taken.shape[1])
    pooled = jnp.sum(blocks, axis=2) / slot_count[:, :, None].astype(jnp.float32)
    pooled = exchange(pooled, 0, 2)[0]
    stats = jnp.stack([jnp.sum(pooled * pooled, axis=1), jnp.max(pooled, axis=1)])
    own = exchange(taken.astype(jnp.bfloat16), 0, 1)
    parcels = [own[:slots]]
    marks = [stats[:, :1]]
    for o in range(1, per_dev):
        parcels.append(shifted(own[o * slots : (o + 1) * slots], ("far", "near"), o))
        marks.append(shifted(stats[:, o : o + 1], ("far", "near"), o))
    marks = jnp.concatenate(marks, axis=1)
    scale = jnp.sqrt(lax.psum(marks[0], "tp") / OUT + EPS)
    return (jnp.concatenate(parcels, axis=0), scale, lax.pmax(marks[1], "tp") / scale)


MESH = pl.DeviceIdType.MESH
LANES = 128
NEAR = 4
FAR = 4


def padded_head(head_dim):
    return -(-head_dim // LANES) * LANES


def norm_rows(value, gain):
    mean = jnp.mean(value, axis=-1, keepdims=True)
    centered = value - mean
    spread = jnp.mean(centered * centered, axis=-1, keepdims=True)
    return (centered * lax.rsqrt(spread + EPS) * gain).astype(jnp.bfloat16)


def dot_nt(left, right):
    return lax.dot_general(left, right, (((1,), (1,)), ((), ())), preferred_element_type=jnp.float32)


def layer_kernel(
    dims,
    grid_h_ref,
    grid_w_ref,
    owner_ref,
    segment_ref,
    mask_ref,
    gain1_ref,
    gain2_ref,
    gain3_ref,
    tok_in,
    qkv_in,
    out_in,
    fc1_in,
    fc2_in,
    proj_in,
    emb_ref,
    norm_ref,
    top_ref,
    qkv_land,
    out_land,
    fc1_land,
    fc2_land,
    proj_land,
    ha,
    hb,
    w_a,
    w_b,
    w_p,
    ids_all,
    qkv_buf,
    att_buf,
    mix,
    hid,
    send,
    acc,
    core_land,
    attn_land,
    rs_land,
    resid,
    picked,
    tok,
    emb_buf,
    tile_buf,
    stat_land,
    wa_s,
    wa_r,
    wl,
    b_s,
    b_r,
    c_s,
    c_r,
    o_s,
    o_r,
    h_s,
    h_r,
    k_s,
    k_r,
    i_s,
    i_r,
    m_s,
    m_r,
    ca_s,
    ca_r,
    cr_s,
    cr_r,
    rr_s,
    rr_r,
    e_s,
    e_r,
    t_s,
    t_r,
    ld,
):
    half, width, hp, heads, slots = dims
    z = lax.axis_index("far")
    q = lax.axis_index("near")
    c = lax.axis_index("tp")
    other = 1 - c
    ahead = lax.rem(z + 1, FAR)
    behind = lax.rem(z + FAR - 1, FAR)
    opposite = lax.rem(z + 2, FAR)
    rows = 2 * half
    places = half // 2
    scale = math.sqrt(HD)

    def peer(d):
        return lax.rem(q + d, NEAR)

    def source(d):
        return lax.rem(q + NEAR - d, NEAR)

    def remote(src, dst, s, r, device):
        return pltpu.make_async_remote_copy(
            src_ref=src, dst_ref=dst, send_sem=s, recv_sem=r, device_id=device, device_id_type=MESH
        )

    def rows_of(ref, first, count, step):
        return ref.at[pl.ds(pl.multiple_of(first, step), count)]

    depth = fc1_in.shape[0]
    piece = (
        lambda n: qkv_in.at[n],
        lambda n: fc1_in.at[:, pl.ds(pl.multiple_of(n * w_a.shape[1], LANES), w_a.shape[1])],
        lambda n: fc2_in.at[:, pl.ds(pl.multiple_of(n * w_b.shape[1], LANES), w_b.shape[1])],
        lambda n: proj_in.at[:, pl.ds(pl.multiple_of(n * w_p.shape[2], LANES), w_p.shape[2])],
    )
    lands = (qkv_land, fc1_land, fc2_land, proj_land)
    deep = (depth, depth, depth, proj_in.shape[0])

    def near_copy(w, d):
        dst = rows_of(lands[w], deep[w] * (NEAR * z + q), deep[w], 8)
        return remote(piece[w](peer(d)), dst, wa_s.at[w, d - 1], wa_r.at[w, d - 1], (z, peer(d), c))

    def near_own(w):
        dst = rows_of(lands[w], deep[w] * (NEAR * z + q), deep[w], 8)
        return pltpu.make_async_copy(piece[w](q), dst, wl.at[w])

    def near_start(w):
        for d in range(1, NEAR):
            near_copy(w, d).start()
        near_own(w).start()

    def near_wait(w):
        for d in range(1, NEAR):
            near_copy(w, d).wait_recv()
        near_own(w).wait()

    items = ((4, 0, 1), (0, 0, 1), (1, 0, 1), (2, 0, 2), (2, 1, 2)) + tuple((3, k, 4) for k in range(4))

    def far_rows(n, place, part, parts):
        w, first, cuts = items[n]
        if w == 4:
            wide = out_land.shape[1] // parts
            start = pl.multiple_of(depth * (NEAR * place + q), 8)
            return out_land.at[pl.ds(start, depth), pl.ds(part * wide, wide)]
        many = NEAR * deep[w] // cuts
        start = NEAR * deep[w] * place + first * many + part * (many // parts)
        return rows_of(lands[w], start, many // parts, 8)

    def far_b(n, way):
        block = far_rows(n, z, 0, 1)
        src = out_in if n == 0 else block
        return remote(src, block, b_s.at[n, way], b_r.at[n, way], ((ahead, behind)[way], q, c))

    def far_c(n, way):
        part = far_rows(n, (behind, ahead)[way], way, 2)
        return remote(part, part, c_s.at[n, way], c_r.at[n, way], ((ahead, behind)[way], q, c))

    def far_start(n):
        for way in (0, 1):
            far_b(n, way).start()

    def far_pass(n):
        for way in (0, 1):
            far_b(n, way).wait_recv()
            far_c(n, way).start()

    def far_wait(n):
        for way in (0, 1):
            far_c(n, way).wait_recv()

    def out_copy(k, d):
        place = (z, behind, ahead, opposite)[k]
        block = far_rows(0, place, 0, 1)
        return remote(out_in if k == 0 else block, block, o_s.at[k, d - 1], o_r.at[k, d - 1], (z, peer(d), c))

    def out_start(k):
        for d in range(1, NEAR):
            out_copy(k, d).start()

    out_own = pltpu.make_async_copy(out_in, far_rows(0, z, 0, 1), wl.at[4])

    def slot(p, core):
        return 2 * p + core

    across = q + 1 - 2 * lax.rem(q, 2)
    along = lax.rem(q + 2, NEAR)
    far_corner = NEAR - 1 - q
    sides = (across, along)
    order = (q, across, along, far_corner)

    def h_half(buf, p, part):
        return buf.at[slot(p, c), pl.ds(part * places, places)]

    def h_copy(ph, buf, side, part):
        block = h_half(buf, q, part)
        return remote(
            block, block, h_s.at[ph, side, part], h_r.at[ph, side, part], (z, sides[side], c)
        )

    def h_relay(ph, buf, side):
        block = h_half(buf, sides[1 - side], 1 - side)
        return remote(block, block, h_s.at[ph, side, 2], h_r.at[ph, side, 2], (z, sides[side], c))

    def h_core(ph, buf, d):
        block = buf.at[slot(order[d], c)]
        return remote(block, block, k_s.at[ph, d], k_r.at[ph, d], (z, q, other))

    def h_start(ph, buf):
        for t in range(2):
            for side in range(2):
                h_copy(ph, buf, side, (side + t) % 2).start()
        h_core(ph, buf, 0).start()

    def h_first(ph, buf):
        for side in range(2):
            h_copy(ph, buf, side, side).wait_recv()
            h_relay(ph, buf, 1 - side).start()

    def h_second(ph, buf):
        for side in range(2):
            h_copy(ph, buf, side, 1 - side).wait_recv()
            h_core(ph, buf, 1 + side).start()

    def h_third(ph, buf):
        for side in range(2):
            h_relay(ph, buf, side).wait_recv()
        h_core(ph, buf, 3).start()

    def h_wait(ph, buf):
        for d in range(NEAR):
            h_core(ph, buf, d).wait_recv()

    def h_done(ph, buf):
        for side in range(2):
            for part in range(2):
                h_copy(ph, buf, side, part).wait_send()
            h_relay(ph, buf, side).wait_send()
        for d in range(NEAR):
            h_core(ph, buf, d).wait_send()

    def ids_copy(d):
        return remote(ids_all.at[q], ids_all.at[q], i_s.at[d - 1], i_r.at[d - 1], (z, peer(d), c))

    load_t = [
        pltpu.make_async_copy(tok_in.at[pl.ds(t * half, half)], hb.at[t], ld.at[5 + t]) for t in range(2)
    ]
    near_start(0)
    far_start(0)
    for t in range(2):
        load_t[t].start()
    out_start(0)
    out_own.start()

    first_row = lax.broadcasted_iota(jnp.int32, (rows, rows), 0)
    first_col = lax.broadcasted_iota(jnp.int32, (rows, rows), 1)
    turn = first_row == 4 * lax.rem(first_col, places) + first_col // places
    segment = segment_ref[...]
    keys = jnp.where(mask_ref[...] > 0, segment, -1)
    line = lax.broadcasted_iota(jnp.int32, (8, rows), 0)
    both = jnp.where(line == 0, segment, keys).astype(jnp.bfloat16)
    ids_all[q] = jnp.dot(both, turn.astype(jnp.bfloat16), preferred_element_type=jnp.float32)
    for d in range(1, NEAR):
        ids_copy(d).start()

    step = 64
    mine = slot(q, c)
    for t in range(2):
        load_t[t].wait()
    run_row = lax.broadcasted_iota(jnp.int32, (places, rows), 0)
    run_col = lax.broadcasted_iota(jnp.int32, (places, rows), 1)
    for j in range(2):
        choose = (run_col == 4 * run_row + (2 * c + j)).astype(jnp.bfloat16)
        got = jnp.dot(choose[:, :half], hb[0], preferred_element_type=jnp.float32)
        got = got + jnp.dot(choose[:, half:], hb[1], preferred_element_type=jnp.float32)
        tok[j * places : (j + 1) * places, :] = got.astype(jnp.bfloat16)

    def first_norm(t, _):
        at = pl.ds(pl.multiple_of(t * step, step), step)
        value = tok[at, :].astype(jnp.float32)
        ha[mine, at, :] = norm_rows(value, gain1_ref[...])
        return 0

    lax.fori_loop(0, half // step, first_norm, 0)
    h_start(0, ha)
    near_wait(0)
    far_start(1)
    near_start(1)
    for way in (0, 1):
        far_b(0, way).wait_recv()
        far_c(0, way).start()
        out_start(1 + way)
    h_first(0, ha)
    h_second(0, ha)
    near_start(2)
    h_third(0, ha)
    far_pass(1)
    near_wait(1)
    far_start(2)
    near_start(3)
    far_wait(0)
    out_start(3)
    near_wait(2)
    far_start(3)
    h_wait(0, ha)
    for d in range(1, NEAR):
        ids_copy(d).wait_recv()
    far_wait(1)

    load_q = pltpu.make_async_copy(qkv_land, w_a.at[:, pl.ds(0, qkv_land.shape[1])], ld.at[0])
    load_q.start()
    load_q.wait()
    triple = qkv_land.shape[1]

    def qkv_rows(s, _):
        got = ha[s]
        for n in range(triple // 256):
            part = jnp.dot(got, w_a[:, n * 256 : (n + 1) * 256], preferred_element_type=jnp.float32)
            qkv_buf[s, :, n * 256 : (n + 1) * 256] = part.astype(jnp.bfloat16)
        return 0

    lax.fori_loop(0, 2 * NEAR, qkv_rows, 0)

    group = heads * hp

    def mix_copy(d):
        lanes = pl.ds(pl.multiple_of(q * group, LANES), group)
        return remote(
            att_buf.at[peer(d)], mix.at[:, lanes], m_s.at[d - 1], m_r.at[d - 1], (z, peer(d), c)
        )

    def attend_rows(p, h, t):
        query = qkv_buf[2 * p + t, :, h * hp : (h + 1) * hp]
        keys = qkv_buf[pl.ds(2 * p, 2), :, group + h * hp : group + (h + 1) * hp]
        values = qkv_buf[pl.ds(2 * p, 2), :, 2 * group + h * hp : 2 * group + (h + 1) * hp]
        scores = dot_nt(query, keys.reshape(rows, hp)) / scale
        segment = jnp.transpose(ids_all[p, :, t * half : (t + 1) * half])[:, 0:1]
        key_ids = ids_all[p, 1:2, :]
        place = lax.broadcasted_iota(jnp.int32, (half, rows), 0) + t * half
        column = lax.broadcasted_iota(jnp.int32, (half, rows), 1)
        visible = (segment == key_ids) | (place == column)
        scores = jnp.where(visible, scores, -1e30)
        peak = jnp.max(scores, axis=-1, keepdims=True)
        weights = jnp.exp(scores - peak)
        total = jnp.sum(weights, axis=-1, keepdims=True)
        probs = (weights / total).astype(jnp.bfloat16)
        mixed = jnp.dot(probs, values.reshape(rows, hp), preferred_element_type=jnp.float32)
        att_buf[p, t * half : (t + 1) * half, h * hp : (h + 1) * hp] = mixed.astype(jnp.bfloat16)

    for d in (1, 2, 3, 0):
        target = peer(d)
        for h in range(heads):
            for t in range(2):
                attend_rows(target, h, t)
        if d:
            mix_copy(d).start()
    mix[:, pl.ds(pl.multiple_of(q * group, LANES), group)] = att_buf[q]

    for k in range(4):
        for d in range(1, NEAR):
            out_copy(k, d).wait_recv()
    out_own.wait()
    load_o = pltpu.make_async_copy(out_land, w_b, ld.at[1])
    load_o.start()
    load_o.wait()
    for d in range(1, NEAR):
        mix_copy(d).wait_recv()

    tile = 128
    tiles = width // tile

    def attn_copy():
        return remote(send.at[0], attn_land, ca_s.at[0], ca_r.at[0], (z, q, other))

    def out_rows(dst, core):
        got = mix[pl.ds(pl.multiple_of(core * half, 16), half), :]
        for n in range(tiles):
            dst[:, n * tile : (n + 1) * tile] = dot_nt(got, w_b[n * tile : (n + 1) * tile, :])

    out_rows(send.at[0], other)
    attn_copy().start()
    out_rows(resid, c)
    h_done(0, ha)
    attn_copy().wait_recv()

    def second_norm(t, _):
        at = pl.ds(pl.multiple_of(t * step, step), step)
        value = tok[at, :].astype(jnp.float32) + (resid[at, :] + attn_land[at, :])
        resid[at, :] = value
        hb[mine, at, :] = norm_rows(value, gain2_ref[...])
        return 0

    lax.fori_loop(0, half // step, second_norm, 0)
    h_start(1, hb)
    far_pass(2)
    far_start(4)
    h_first(1, hb)
    h_second(1, hb)
    far_pass(3)
    near_wait(3)
    far_start(5)
    h_third(1, hb)
    far_wait(2)
    load_1 = pltpu.make_async_copy(fc1_land, w_a, ld.at[2])
    load_1.start()
    load_1.wait()
    h_wait(1, hb)
    hidden = w_a.shape[1]

    def fc1_rows(s, _):
        got = hb[s]
        for n in range(hidden // 256):
            part = jnp.dot(got, w_a[:, n * 256 : (n + 1) * 256], preferred_element_type=jnp.float32)
            part = 0.5 * part * (1.0 + lax.erf(part * math.sqrt(0.5)))
            hid[s, :, n * 256 : (n + 1) * 256] = part.astype(jnp.bfloat16)
        return 0

    lax.fori_loop(0, 2 * NEAR, fc1_rows, 0)
    h_done(1, hb)
    attn_copy().wait_send()

    far_pass(4)
    far_start(6)
    far_wait(3)
    far_wait(4)
    load_2 = pltpu.make_async_copy(fc2_land, w_b, ld.at[3])
    load_2.start()
    load_2.wait()

    def fc2_rows(dst, s):
        got = hid[s]
        for n in range(tiles):
            dst[:, n * tile : (n + 1) * tile] = dot_nt(got, w_b[n * tile : (n + 1) * tile, :])

    turns = (3, 1, 2, 0)

    def core_copy(i):
        return remote(send.at[i % 2], core_land.at[i], cr_s.at[i], cr_r.at[i], (z, q, other))

    def rs_copy(k):
        side, d, part = ((0, 3, 0), (1, 3, 1), (0, 1, 0), (1, 2, 1), (1, 2, 0), (0, 1, 1))[k]
        src = acc.at[d, pl.ds(part * places, places)]
        return remote(src, rs_land.at[k], rr_s.at[k], rr_r.at[k], (z, sides[side], c))

    def join(i):
        core_copy(i).wait_recv()

        def add(t, _):
            at = pl.ds(pl.multiple_of(t * step, step), step)
            acc[turns[i], at, :] = acc[turns[i], at, :] + core_land[i, at, :]
            return 0

        lax.fori_loop(0, half // step, add, 0)

    def relay(d, part, k):
        rs_copy(k).wait_recv()

        def add(t, _):
            at = pl.ds(pl.multiple_of(part * places + t * step, step), step)
            acc[d, at, :] = acc[d, at, :] + rs_land[k, pl.ds(pl.multiple_of(t * step, step), step), :]
            return 0

        lax.fori_loop(0, places // step, add, 0)

    for i in range(4):
        target = order[turns[i]]
        if i >= 2:
            core_copy(i - 2).wait_send()
        fc2_rows(send.at[i % 2], slot(target, other))
        core_copy(i).start()
        fc2_rows(acc.at[turns[i]], slot(target, c))
        join(i)
        if i == 0:
            rs_copy(0).start()
            rs_copy(1).start()
        elif i < 3:
            rs_copy(1 + i).start()

    relay(1, 1, 1)
    rs_copy(5).start()
    relay(2, 0, 0)
    rs_copy(4).start()
    far_pass(5)
    far_start(7)
    far_pass(6)
    far_start(8)
    for k in range(2, 6):
        rs_copy(k).wait_recv()

    for part in range(2):

        def third_norm(t, _):
            at = pl.ds(pl.multiple_of(part * places + t * step, step), step)
            near_at = pl.ds(pl.multiple_of(t * step, step), step)
            sums = acc[0, at, :] + rs_land[2 + part, near_at, :] + rs_land[4 + part, near_at, :]
            picked[at, :] = norm_rows(resid[at, :] + sums, gain3_ref[...])
            return 0

        lax.fori_loop(0, places // step, third_norm, 0)

    def lengths(p):
        got = []
        for k in range(2):
            r = 2 * (NEAR * z + p) + k
            got.append(grid_h_ref[r] * grid_w_ref[r] // 4)
        shift = owner_ref[2 * (NEAR * z + p)] - (NEAR * z + p)
        return got[0], got[1], (shift == 0)

    one, two, straight = lengths(q)
    run = lax.broadcasted_iota(jnp.int32, (places, places), 0)
    col = lax.broadcasted_iota(jnp.int32, (places, places), 1)
    top = run < slots
    taken = run - jnp.where(top, 0, slots)
    first_req = top == straight
    count = jnp.where(first_req, one, two)
    sel = ((col == taken + jnp.where(first_req, 0, one)) & (taken < count)).astype(jnp.bfloat16)
    quarter = half // 2
    for j in range(2):
        got = jnp.dot(
            sel, picked[j * quarter : (j + 1) * quarter, :], preferred_element_type=jnp.float32
        )
        ha[mine, j * quarter : (j + 1) * quarter, :] = got.astype(jnp.bfloat16)
    h_start(2, ha)
    far_pass(7)
    h_first(2, ha)
    h_second(2, ha)
    far_pass(8)
    h_third(2, ha)

    def load_p(k):
        first = pl.multiple_of(width * (z, behind, ahead, opposite)[k], 16)
        return pltpu.make_async_copy(proj_land.at[pl.ds(first, width)], w_p.at[k], ld.at[(4, 3, 2, 1)[k]])

    for k in range(3):
        load_p(k).start()
    h_wait(2, ha)
    for k in range(6):
        rs_copy(k).wait_send()
    wide = w_p.shape[2]
    cols = pl.ds(pl.multiple_of(q * wide, LANES), wide)

    def emb_copy(o, d):
        at = pl.ds(o * slots, slots)
        if o == 0:
            device = (z, peer(d), c)
            src = emb_buf.at[peer(d), at]
        else:
            owner = peer(d)
            step_z = 1 - jnp.minimum(owner, 1)
            device = (lax.rem(z + step_z, FAR), owner, c)
            src = emb_buf.at[lax.rem(owner + NEAR - 1, NEAR), at]
        return remote(src, emb_ref.at[at, cols], e_s.at[o, d], e_r.at[o, d], device)

    def emb_own(o):
        at = pl.ds(o * slots, slots)
        src = emb_buf.at[q if o == 0 else lax.rem(q + NEAR - 1, NEAR), at]
        return pltpu.make_async_copy(src, emb_ref.at[at, cols], wl.at[5 + o])

    def stat_copy(o, d, k):
        owner = peer(d)
        core = c if k == 0 else other
        if o == 0:
            device = (z, owner, core)
            src = tile_buf.at[owner, 0]
        else:
            step_z = 1 - jnp.minimum(owner, 1)
            device = (lax.rem(z + step_z, FAR), owner, core)
            src = tile_buf.at[lax.rem(owner + NEAR - 1, NEAR), 1]
        return remote(src, stat_land.at[o, mine], t_s.at[o, d, k], t_r.at[o, d, k], device)

    def proj_part(k, p):
        place = (z, behind, ahead, opposite)[k]
        part = pl.ds(pl.multiple_of(lax.rem(place, 2) * quarter, quarter), quarter)
        got = ha[2 * p + place // 2, part, :]
        return jnp.dot(got, w_p[k], preferred_element_type=jnp.float32)

    def proj_rows(p, _):
        total = proj_part(0, p) + proj_part(1, p) + proj_part(2, p)
        acc[p, 0:quarter, 0:wide] = total
        return 0

    def last_rows(p, _):
        total = acc[p, 0:quarter, 0:wide] + proj_part(3, p)
        emb_buf[p] = total.astype(jnp.bfloat16)
        one, two, straight = lengths(p)
        for o in range(2):
            count = jnp.where(straight, (one, two)[o], (two, one)[o]).astype(jnp.float32)
            pooled = jnp.sum(total[o * slots : (o + 1) * slots], axis=0, keepdims=True) / count
            squares = jnp.sum(pooled * pooled, axis=1, keepdims=True)
            largest = jnp.max(pooled, axis=1, keepdims=True)
            line = lax.broadcasted_iota(jnp.int32, (8, LANES), 0)
            tile_buf[p, o] = jnp.where(line == 0, squares, largest)
        return 0

    for k in range(3):
        load_p(k).wait()
    lax.fori_loop(0, NEAR, proj_rows, 0)
    for n in range(5, 9):
        far_wait(n)
    load_p(3).start()
    load_p(3).wait()
    lax.fori_loop(0, NEAR, last_rows, 0)

    for d in range(1, NEAR):
        for o in range(2):
            emb_copy(o, d).start()
            for k in range(2):
                stat_copy(o, d, k).start()
    emb_own(0).start()
    stat_land[0, mine] = tile_buf[q, 0]
    stat_copy(0, 0, 1).start()
    stat_copy(1, 0, 1).start()

    @pl.when(q == 0)
    def _():
        emb_copy(1, 0).start()
        stat_copy(1, 0, 0).start()

    @pl.when(q != 0)
    def _():
        emb_own(1).start()
        stat_land[1, mine] = tile_buf[lax.rem(q + NEAR - 1, NEAR), 1]
        emb_own(1).wait()

    emb_own(0).wait()
    for d in range(1, NEAR):
        for o in range(2):
            emb_copy(o, d).wait()
            for k in range(2):
                stat_copy(o, d, k).wait()
    stat_copy(0, 0, 1).wait()
    stat_copy(1, 0, 1).wait()

    @pl.when(q == 0)
    def _():
        emb_copy(1, 0).wait()
        stat_copy(1, 0, 0).wait()

    features = wide * NEAR * 2
    for o in range(2):
        squares = jnp.zeros((1, LANES), jnp.float32)
        largest = stat_land[o, 0, 1:2, :]
        for s in range(2 * NEAR):
            squares = squares + stat_land[o, s, 0:1, :]
            largest = jnp.maximum(largest, stat_land[o, s, 1:2, :])
        norm = jnp.sqrt(squares / features + EPS)
        norm_ref[o] = jnp.max(norm)
        top_ref[o] = jnp.max(largest / norm)

    for w in range(4):
        for d in range(1, NEAR):
            near_copy(w, d).wait_send()
    for n in range(len(items)):
        for way in (0, 1):
            far_b(n, way).wait_send()
            far_c(n, way).wait_send()
    for k in range(4):
        for d in range(1, NEAR):
            out_copy(k, d).wait_send()
    for d in range(1, NEAR):
        ids_copy(d).wait_send()
        mix_copy(d).wait_send()
    for i in (2, 3):
        core_copy(i).wait_send()
    h_done(2, ha)


def kernel_shards(
    tokens,
    qkv_weight,
    out_weight,
    fc1_weight,
    fc2_weight,
    norm1_gain,
    norm2_gain,
    norm3_gain,
    proj_weight,
    grid_h,
    grid_w,
    segment_ids,
    patch_mask,
    owner,
):
    rows, width = tokens.shape
    half = rows // 2
    places = rows // 4
    slots = places // 2
    hp = padded_head(HD)
    depth = qkv_weight.shape[0]
    all_heads = qkv_weight.shape[2] // HD
    heads = all_heads // NEAR

    extra = ((0, 0),) * 4 + ((0, hp - HD),)
    cut = jnp.pad(qkv_weight.reshape(depth, 3, NEAR, heads, HD), extra)
    cut = cut.transpose(2, 0, 1, 3, 4).reshape(NEAR, depth, 3 * heads * hp)
    out_t = jnp.pad(out_weight.T.reshape(depth, all_heads, HD), extra[:2] + extra[-1:])
    out_t = out_t.reshape(depth, all_heads * hp)
    fc2_t = fc2_weight.T

    hidden = fc1_weight.shape[1] // NEAR
    wide = proj_weight.shape[1] // NEAR
    bf16, f32 = jnp.bfloat16, jnp.float32
    shape = jax.ShapeDtypeStruct
    vmem = pl.BlockSpec(memory_space=pltpu.VMEM)
    smem = pl.BlockSpec(memory_space=pltpu.SMEM)
    anyw = pl.BlockSpec(memory_space=pl.ANY)
    dma = pltpu.SemaphoreType.DMA
    outs = pl.pallas_call(
        functools.partial(layer_kernel, (half, width, hp, heads, slots)),
        out_shape=(
            shape((places, proj_weight.shape[1]), bf16),
            shape((2,), f32),
            shape((2,), f32),
            shape((width, cut.shape[2]), bf16),
            shape((width, out_t.shape[1]), bf16),
            shape((width, hidden), bf16),
            shape((width, hidden), bf16),
            shape((4 * width, wide), bf16),
        ),
        in_specs=[smem] * 3 + [vmem] * 5 + [anyw] * 6,
        out_specs=(anyw, smem, smem) + (anyw,) * 5,
        scratch_shapes=[
            pltpu.VMEM((2 * NEAR, half, width), bf16),
            pltpu.VMEM((2 * NEAR, half, width), bf16),
            pltpu.VMEM((width, hidden), bf16),
            pltpu.VMEM((width, hidden), bf16),
            pltpu.VMEM((4, width, wide), bf16),
            pltpu.VMEM((NEAR, 8, rows), f32),
            pltpu.VMEM((2 * NEAR, half, cut.shape[2]), bf16),
            pltpu.VMEM((NEAR, rows, heads * hp), bf16),
            pltpu.VMEM((rows, all_heads * hp), bf16),
            pltpu.VMEM((2 * NEAR, half, hidden), bf16),
            pltpu.VMEM((2, half, width), f32),
            pltpu.VMEM((NEAR, half, width), f32),
            pltpu.VMEM((NEAR, half, width), f32),
            pltpu.VMEM((half, width), f32),
            pltpu.VMEM((6, places, width), f32),
            pltpu.VMEM((half, width), f32),
            pltpu.VMEM((half, width), bf16),
            pltpu.VMEM((half, width), bf16),
            pltpu.VMEM((NEAR, places, wide), bf16),
            pltpu.VMEM((NEAR, 2, 8, LANES), f32),
            pltpu.VMEM((2, 2 * NEAR, 8, LANES), f32),
            dma((4, 3)),
            dma((4, 3)),
            dma((7,)),
            dma((9, 2)),
            dma((9, 2)),
            dma((9, 2)),
            dma((9, 2)),
            dma((4, 3)),
            dma((4, 3)),
            dma((3, 2, 3)),
            dma((3, 2, 3)),
            dma((3, 4)),
            dma((3, 4)),
            dma((3,)),
            dma((3,)),
            dma((3,)),
            dma((3,)),
            dma((1,)),
            dma((1,)),
            dma((4,)),
            dma((4,)),
            dma((6,)),
            dma((6,)),
            dma((2, 4)),
            dma((2, 4)),
            dma((2, 4, 2)),
            dma((2, 4, 2)),
            dma((7,)),
        ],
        compiler_params=pltpu.CompilerParams(vmem_limit_bytes=67043328, has_side_effects=True),
        name="layer",
    )(
        grid_h,
        grid_w,
        owner,
        segment_ids[None],
        patch_mask[None],
        norm1_gain[None],
        norm2_gain[None],
        norm3_gain[None],
        tokens,
        cut,
        out_t,
        fc1_weight,
        fc2_t,
        proj_weight,
    )
    return outs[0], outs[1], outs[2]


def group_of(mesh, args):
    tp, req = mesh.shape["tp"], mesh.shape["req"]
    for near in (4, 2):
        whole = req % near == 0
        heads = args[1].shape[2] // (HD * tp)
        if whole and heads % near == 0:
            return near
    return 1


def solution(mesh):
    def step(*args):
        near = group_of(mesh, args)
        if near == 1:
            return plain_solution(mesh)(*args)
        tp, req = mesh.shape["tp"], mesh.shape["req"]
        split = jax.sharding.Mesh(
            mesh.devices.reshape(req // near, near, tp), ("far", "near", "tp")
        )
        both = ("far", "near")
        whole = tp == 2 and near == NEAR and req == NEAR * FAR and args[9].shape[0] == 2 * req
        return jax.shard_map(
            kernel_shards if whole else grouped_shards,
            mesh=split,
            in_specs=(
                P(both, None),
                P(both, None, "tp"),
                P("tp", both),
                P(both, "tp"),
                P("tp", both),
                P(),
                P(),
                P(),
                P(both, "tp"),
                P(),
                P(),
                P(both),
                P(both),
                P(),
            ),
            out_specs=(P(both, "tp"), P(both), P(both)),
            check_vma=False,
        )(*args)

    return step
```
